256 devices in a mesh: dp: 16 (over x, y_hi, core), tensor: 16 (over y_lo, z).
Axes of the slice: x: 4, y: 4 (y_hi: 2, y_lo: 2; y = y_hi * 2 + y_lo), z: 8, core: 2. Of those that a mesh axis runs over, the one named last changes fastest.
Arguments:
- enc_hidden: bfloat16 [32768, 4096], P(('dp', 'tensor')), parts along dimension 0, may hold values from -6 to 6
- enc_gain: float32 [4096], replicated, may hold values from 0.1 to 1.9
- dec_hidden: bfloat16 [8192, 4096], P(('dp', 'tensor')), parts along dimension 0, may hold values from -6 to 6
- dec_gain: float32 [4096], replicated, may hold values from 0.8 to 12, as said below
- w_query: bfloat16 [4096, 4096], P(None, 'tensor'), may hold values from -0.046875 to 0.046875
- w_key: bfloat16 [4096, 4096], P(None, 'tensor'), may hold values from -0.09375 to 0.09375
- w_value: bfloat16 [4096, 4096], P(None, 'tensor'), may hold values from -0.09375 to 0.09375
- w_out: bfloat16 [4096, 4096], P('tensor'), may hold values from -0.75 to 0.75
- enc_length: int32 [16], P('dp'), parts along dimension 0, may hold values from 1024 to 2048
- dec_length: int32 [16], P('dp'), parts along dimension 0, may hold values from 256 to 512
Outputs:
- memory: bfloat16 [32768, 4096], P(('dp', 'tensor')), parts along dimension 0
- cross_out: bfloat16 [8192, 4096], P(('dp', 'tensor')), parts along dimension 0
The draws below stay inside these ranges and needn't reach their ends.
There are 16 independent parts, one for each index of `dp`. The reference program is written for one: setup_inputs(seed, part) draws one part's arguments, and reference() takes and returns one part's arrays. A program takes and returns all parts, laid end to end along the dimension named above; an argument that names none is the same for every part. Nothing has to cross between parts.
Inputs may be any that keep to these rules, and one draw needn't show every extreme that they name: `dec_gain`: positive.
All inputs are finite; a program needn't handle non-finite values.
Results may differ from the reference program's by a relative error of at most 0.02.
The reference program's roundings to bfloat16 on the way count: a program that leaves them out, or rounds other values in their place, can miss the bound.
Values may be sent and summed in bfloat16 or wider, within the bound.
A program may use at most 128 MiB of HBM per device.

```python
import jax
import jax.numpy as jnp
from jax import lax

D = 4096
HEADS = 64
HEAD_DIM = 64
ENC_LEN = 2048
DEC_LEN = 512
HD = 4096
N_TENSOR = 16


def draw_dec_gain(key, part):
    return jax.random.uniform(key, (D,), jnp.float32, 0.8, 1.2)


def levels(key, extent, split, low, high):
    def one(position, parts):
        heights = jax.random.uniform(jax.random.fold_in(jax.random.fold_in(key, 6), position), (parts,), jnp.float32, low / len(split), high / len(split))
        return jnp.repeat(jnp.exp(heights), extent[position] // parts).reshape((-1,) + (1,) * (len(extent) - position - 1))

    factor_of = one(*split[0])
    for cut in split[1:]:
        factor_of = factor_of * one(*cut)
    return factor_of


def noise(rng, shape, scale, limit, split=(), kind=jnp.bfloat16):
    level = levels(rng, shape, split, -0.22, 0.18) if split else 1.0
    array = jax.random.normal(rng, shape, jnp.float32) * scale * level
    return jnp.minimum(jnp.maximum(array, -limit), limit).astype(kind)


def setup_inputs(seed: int = 0, part: int = 0) -> dict:
    streams_of = jax.random.split(jax.random.key(seed), 11)
    part_splits = jax.random.split(jax.random.fold_in(streams_of[10], part), 11)
    return {
        "enc_hidden": noise(part_splits[0], (ENC_LEN, D), 1.0, 6.0, ((0, 16),)),
        "enc_gain": jnp.clip(1.0 + 0.18 * jax.random.normal(streams_of[1], (D,), jnp.float32), 0.1, 1.9),
        "dec_hidden": noise(part_splits[2], (DEC_LEN, D), 1.0, 6.0, ((0, 16),)),
        "dec_gain": draw_dec_gain(jax.random.fold_in(streams_of[10], 71), part),
        "w_query": noise(streams_of[4], (D, HD), (4 * D) ** -0.5, 0.046875, ((1, 16),)),
        "w_key": noise(streams_of[5], (D, HD), D ** -0.5, 0.09375, ((1, 16),)),
        "w_value": noise(streams_of[6], (D, HD), D ** -0.5, 0.09375, ((1, 16),)),
        "w_out": noise(streams_of[7], (HD, D), HEAD_DIM ** -0.5, 0.75, ((0, 16),)),
        "enc_length": jax.random.randint(part_splits[8], (1,), ENC_LEN // 2, ENC_LEN + 1).astype(jnp.int32),
        "dec_length": jax.random.randint(part_splits[9], (1,), DEC_LEN // 2, DEC_LEN + 1).astype(jnp.int32),
    }


def rms_norm(values, gain):
    wide = values.astype(jnp.float32)
    mean_sq = lax.optimization_barrier(jnp.mean(wide * wide, axis=-1, keepdims=True))
    return (wide * jax.lax.rsqrt(mean_sq + 1e-06) * gain.astype(jnp.float32)).astype(jnp.bfloat16)

def reference(enc_hidden, enc_gain, dec_hidden, dec_gain, w_query, w_key, w_value, w_out, enc_length, dec_length):
    memory = rms_norm(enc_hidden, enc_gain)
    normed = rms_norm(dec_hidden, dec_gain)
    queries = jnp.dot(normed, w_query, preferred_element_type=jnp.float32).astype(jnp.bfloat16)
    key_rows = jnp.dot(memory, w_key, preferred_element_type=jnp.float32).astype(jnp.bfloat16)
    value_rows = jnp.dot(memory, w_value, preferred_element_type=jnp.float32).astype(jnp.bfloat16)
    q_heads = queries.reshape(DEC_LEN, HEADS, HEAD_DIM).astype(jnp.float32)
    k_heads = key_rows.reshape(ENC_LEN, HEADS, HEAD_DIM).astype(jnp.float32)
    v_heads = value_rows.reshape(ENC_LEN, HEADS, HEAD_DIM).astype(jnp.float32)
    scores = jnp.einsum('qhd,khd->hqk', q_heads, k_heads)
    valid_keys = jnp.arange(ENC_LEN, dtype=jnp.int32) < enc_length[0]
    scores = jnp.where(valid_keys[None, None, :], scores, -jnp.inf)
    weights = jax.nn.softmax(scores, axis=-1).astype(jnp.bfloat16)
    context = jnp.einsum('hqk,khd->qhd', weights.astype(jnp.float32), v_heads)
    context = context.astype(jnp.bfloat16).reshape(DEC_LEN, HD)
    group_width = HD // N_TENSOR
    context_groups = context.reshape(DEC_LEN, N_TENSOR, group_width).transpose(1, 0, 2)
    out_groups = w_out.reshape(N_TENSOR, group_width, D)

    def add_group(total, pair):
        ctx_part, out_part = pair
        partial_value = jnp.dot(ctx_part, out_part, preferred_element_type=jnp.float32)
        partial_value = partial_value.astype(jnp.bfloat16).astype(jnp.float32)
        return (total + partial_value, None)
    projected, _ = lax.scan(add_group, jnp.zeros((DEC_LEN, D), jnp.float32), (context_groups, out_groups))
    live_rows = jnp.arange(DEC_LEN, dtype=jnp.int32) < dec_length[0]
    cross_out = jnp.where(live_rows[:, None], projected, 0.0).astype(jnp.bfloat16)
    return (memory, cross_out)
```

```python
import functools

import jax
import jax.numpy as jnp
from jax import lax
from jax.experimental import pallas as pl
from jax.experimental.pallas import tpu as pltpu
from jax.sharding import Mesh
from jax.sharding import PartitionSpec as P

HEAD_DIM = 64
MESH = pl.DeviceIdType.MESH
NZ = 8
NEG = -1e30
ROWS = ("x", "yh", "c", "yl", "z")
BF16, F32 = jnp.bfloat16, jnp.float32

R_ITEMS = (
    [("n", 0, 0), ("m", 0, 0), ("n", 1, 0), ("m", 0, 1), ("n", 2, 0), ("m", 0, 2), ("n", 3, 0), ("m", 0, 3)]
    + [("m", 1, p) for p in range(4)]
    + [("m", 2, p) for p in range(4)]
    + [("m", 3, 0)]
)
L_ITEMS = (
    [("n", 0, 0), ("m", 0, 0), ("n", 1, 0), ("m", 0, 1), ("n", 2, 0), ("m", 0, 2), ("m", 0, 3)]
    + [("m", 1, p) for p in range(4)]
    + [("m", 2, p) for p in range(4)]
    + [("m", 3, p) for p in (1, 2, 3)]
)


def schedule(items):
    after, last = {}, -1
    for i, (kind, hop, piece) in enumerate(items):
        need = items.index((kind, hop - 1, piece)) if hop else -1
        last = max(last, need)
        after.setdefault(last, []).append(i)
    return after


def kernel(
    len_ref, n_hbm, m_hbm, wq_hbm, wk_hbm, wv_hbm, wo_hbm, out_ref,
    gn, gm, w, wo, kv, q, qtm, vt, acc, mx, sm, ctx, prod, rs_send, rs_recv,
    loc, z_send, z_recv, wy_send, wy_recv, xa_send, xa_recv, xb_send, xb_recv, c_send, c_recv,
    q_sem, kv_send, kv_recv, rss, rsr,
):
    x, c = lax.axis_index("x"), lax.axis_index("c")
    y, z = lax.axis_index("yl"), lax.axis_index("z")
    yn, cn = 1 - y, 1 - c
    xa, xb = x + 1 - 2 * (x % 2), 3 - x
    right, left = (z + 1) % NZ, (z + NZ - 1) % NZ
    peers = ({"z": right}, {"z": left}, {"yl": yn}, {"x": xa}, {"x": xb}, {"c": cn})

    barrier = pltpu.get_barrier_semaphore()
    for peer in peers:
        pl.semaphore_signal(barrier, inc=1, device_id=peer, device_id_type=MESH)
    pl.semaphore_wait(barrier, len(peers))

    def remote(src, dst, ssem, rsem, peer):
        return pltpu.make_async_remote_copy(
            src_ref=src, dst_ref=dst, send_sem=ssem, recv_sem=rsem, device_id=peer, device_id_type=MESH
        )

    def z_ref(kind, owner, piece):
        return gn.at[owner] if kind == "n" else gm.at[owner, pl.ds(32 * piece, 32), :]

    def z_copy(d, i, receive):
        kind, hop, piece = (R_ITEMS, L_ITEMS)[d][i]
        shift = hop + (1 if receive else 0)
        owner = (z + (NZ - shift if d == 0 else shift)) % NZ
        dst = z_ref(kind, owner, piece)
        src = dst
        if hop == 0 and not receive:
            src = n_hbm if kind == "n" else m_hbm.at[pl.ds(32 * piece, 32), :]
        return remote(src, dst, z_send.at[d, i], z_recv.at[d, i], peers[d])

    plan = (schedule(R_ITEMS), schedule(L_ITEMS))

    def z_issue(d, k):
        for i in plan[d].get(k, ()):
            z_copy(d, i, False).start()

    def serve(d, k):
        z_copy(d, k, True).wait_recv()
        z_issue(d, k)

    hbm = (wk_hbm, wv_hbm, wq_hbm, wo_hbm)
    STEP = (512, 512, 512, 32)

    def part(t, e, n=1):
        rows = pl.ds(e * STEP[t], n * STEP[t])
        return wo.at[1, rows, :] if t == 3 else w.at[1, t, rows, :]

    mine = c * 4 + x

    def wy(t):
        src = hbm[t].at[pl.ds(mine * STEP[t], STEP[t]), :]
        return remote(src, part(t, mine), wy_send.at[t], wy_recv.at[t], peers[2])

    def wxa(t, receive=False):
        r = part(t, c * 4 + (xa if receive else x))
        return remote(r, r, xa_send.at[t], xa_recv.at[t], peers[3])

    def wxb(t, k, receive=False):
        near, far = (xb, xb + 1 - 2 * (xb % 2)) if receive else (x, xa)
        r = part(t, c * 4 + (far if k else near))
        return remote(r, r, xb_send.at[t, k], xb_recv.at[t, k], peers[4])

    def wc(t, receive=False):
        r = part(t, 4 * (cn if receive else c), 4)
        return remote(r, r, c_send.at[t], c_recv.at[t], peers[5])

    def got_y(t):
        wy(t).wait_recv()
        wxb(t, 0).start()
        wxa(t).start()

    def got_xa(t):
        wxa(t, True).wait_recv()
        wxb(t, 1).start()

    def got_xb(t):
        wxb(t, 0, True).wait_recv()
        wxb(t, 1, True).wait_recv()
        wc(t).start()

    for d in (0, 1):
        z_issue(d, -1)
    for t in range(4):
        wy(t).start()
    local = [
        pltpu.make_async_copy(n_hbm, gn.at[z], loc.at[0]),
        pltpu.make_async_copy(m_hbm, gm.at[z], loc.at[1]),
        pltpu.make_async_copy(wk_hbm, w.at[0, 0], loc.at[2]),
        pltpu.make_async_copy(wv_hbm, w.at[0, 1], loc.at[3]),
        pltpu.make_async_copy(wq_hbm, w.at[0, 2], loc.at[4]),
        pltpu.make_async_copy(wo_hbm, wo.at[0], loc.at[5]),
    ]
    for copy in local:
        copy.start()
    mx[...] = jnp.full_like(mx, NEG)
    sm[...] = jnp.zeros_like(sm)
    acc[...] = jnp.zeros_like(acc)

    def both(k):
        serve(0, k)
        serve(1, k)

    both(0)
    got_y(0)
    got_y(1)
    got_xa(0)
    both(1)
    got_y(2)
    got_xa(1)
    both(2)
    got_y(3)
    got_xa(2)
    got_xb(0)
    both(3)
    got_xb(1)
    got_xa(3)
    both(4)
    both(5)
    got_xb(2)
    both(6)
    serve(0, 7)
    for copy in local:
        copy.wait()
    for t in (2, 0, 1):
        wc(t, True).wait_recv()

    q_copy = remote(q.at[2], q.at[1], q_sem.at[0], q_sem.at[1], peers[2])
    tokens = gn[...].reshape(NZ * 32, gn.shape[2])

    @pl.loop(0, 2)
    def _(i):
        q[2 - 2 * i] = jnp.dot(tokens, w[1 - i, 2], preferred_element_type=F32).astype(BF16)

    q_copy.start()

    def block_of(j):
        near = (j + 1) // 2
        return (z + NZ + near - 2 * near * (j % 2)) % NZ

    def kv_copy(j):
        zb = block_of(j)
        return remote(kv.at[2, zb], kv.at[1, zb], kv_send.at[j], kv_recv.at[j], peers[2])

    def project(j):
        zb = block_of(j)
        rows = gm[zb]

        @pl.loop(0, 4)
        def _(i):
            own, which = i // 2, i % 2
            kv[2 - 2 * own, zb, which] = jnp.dot(
                rows, w[1 - own, which], preferred_element_type=F32
            ).astype(BF16)

        kv_copy(j).start()

    def attend(j):
        zb = block_of(j)
        kv_copy(j).wait_recv()
        keys = jnp.concatenate([kv[0, zb, 0], kv[1, zb, 0]], axis=0)
        values = jnp.concatenate([kv[0, zb, 1], kv[1, zb, 1]], axis=0)
        vt[...] = values.T
        length = len_ref[0]
        row = lax.broadcasted_iota(jnp.int32, (128, 1), 0)
        index = jnp.concatenate([row + (y * NZ + zb) * 128, row + (yn * NZ + zb) * 128], axis=0)
        valid = jnp.broadcast_to(index, (256, 256)) < length

        @pl.loop(0, 4)
        def _(h):
            v_h = vt[pl.ds(pl.multiple_of(h * 64, 64), 64), :]
            for half in range(2):
                cols = pl.ds(half * 256, 256)
                s = jnp.dot(keys, qtm[h, :, cols], preferred_element_type=F32)
                s = jnp.where(valid, s, NEG)
                old = mx[h, :, cols]
                new = jnp.maximum(old, jnp.max(s, axis=0, keepdims=True))
                p = jnp.exp(s - new)
                scale = jnp.exp(old - new)
                mx[h, :, cols] = new
                sm[h, :, cols] = scale * sm[h, :, cols] + jnp.sum(p, axis=0, keepdims=True)
                acc[h, :, cols] = scale * acc[h, :, cols] + jnp.dot(
                    v_h, p.astype(BF16), preferred_element_type=F32
                )

    project(0)
    q_copy.wait_recv()
    first = jnp.where(y == 0, q[0], q[1])
    second = jnp.where(y == 0, q[1], q[0])
    qt = jnp.concatenate([first.T, second.T], axis=1)
    lane = lax.broadcasted_iota(jnp.int32, (256, 512), 0)
    for h in range(4):
        qtm[h] = jnp.where(lane // HEAD_DIM == h, qt, jnp.zeros_like(qt))

    need = {
        1: [(1, 7), (0, 8)],
        2: [(1, 8), (0, 9)],
        3: [(0, 10), (1, 9), (0, 11), (1, 10)],
        5: [(d, k) for i in range(4) for d, k in ((0, 12 + i), (1, 11 + i))],
        7: [(1, 15), (0, 16), (1, 16), (1, 17)],
    }

    @pl.loop(1, NZ)
    def _(j):
        for jj, todo in need.items():

            @pl.when(j == jj)
            def _():
                for d, k in todo:
                    serve(d, k)

        @pl.when(j == 4)
        def _():
            got_xb(3)

        project(j)
        attend(j - 1)

    attend(NZ - 1)
    wc(3, True).wait_recv()

    full = [(acc[h] * (1.0 / sm[h])).astype(BF16) for h in range(4)]
    full = jnp.concatenate(full, axis=0)
    low, high = full[:, :256].T, full[:, 256:].T
    ctx[2] = jnp.where(y == 0, high, low)
    ctx_copy = remote(ctx.at[2], ctx.at[1], q_sem.at[2], q_sem.at[3], peers[2])
    ctx_copy.start()
    ctx[0] = jnp.where(y == 0, low, high)
    ctx_copy.wait_recv()

    @pl.loop(0, 8)
    def _(i):
        cols = pl.ds(pl.multiple_of(i * 512, 512), 512)
        prod[:, cols] = jnp.dot(ctx[0], wo[0, :, cols], preferred_element_type=F32) + jnp.dot(
            ctx[1], wo[1, :, cols], preferred_element_type=F32
        )

    orders = (
        [(0, 4), (1, 3), (0, 3), (1, 2), (0, 2), (1, 1), (0, 1)],
        [(1, 4), (0, 3), (1, 3), (0, 2), (1, 2), (0, 1), (1, 1)],
    )

    def rs_copy(d, i):
        return remote(rs_send.at[d, i], rs_recv.at[d, i], rss.at[d, i], rsr.at[d, i], peers[d])

    def own_rows(owner, half):
        rows = pl.ds(pl.multiple_of(owner * 32, 32), 32)
        return prod[rows, pl.ds(half * 2048, 2048)]

    for i in range(7):
        for d in (0, 1):
            half, far = orders[d][i]
            owner = (z + (far if d == 0 else NZ - far)) % NZ
            term = own_rows(owner, half)
            if i >= 2:
                rs_copy(d, i - 2).wait_recv()
                term = term + rs_recv[d, i - 2].astype(F32)
            rs_send[d, i] = term.astype(BF16)
            rs_copy(d, i).start()
    for d in (0, 1):
        for i in (5, 6):
            rs_copy(d, i).wait_recv()
    for half in (0, 1):
        total = own_rows(z, half)
        total = total + rs_recv[0, 6 - half].astype(F32) + rs_recv[1, 5 + half].astype(F32)
        out_ref[:, pl.ds(half * 2048, 2048)] = total.astype(BF16)

    for d in (0, 1):
        for i in range(len((R_ITEMS, L_ITEMS)[d])):
            z_copy(d, i, False).wait_send()
        for i in range(7):
            rs_copy(d, i).wait_send()
    for t in range(4):
        wy(t).wait_send()
        wxa(t).wait_send()
        wxb(t, 0).wait_send()
        wxb(t, 1).wait_send()
        wc(t).wait_send()
    q_copy.wait_send()
    ctx_copy.wait_send()
    for j in range(NZ):
        kv_copy(j).wait_send()


def rms_norm(values, gain):
    wide = values.astype(F32)
    mean_sq = jnp.mean(wide * wide, axis=-1, keepdims=True)
    return (wide * lax.rsqrt(mean_sq + 1e-06) * gain).astype(BF16)


def shards(enc_hidden, enc_gain, dec_hidden, dec_gain, w_query, w_key, w_value, w_out, enc_length, dec_length):
    memory = rms_norm(enc_hidden, enc_gain)
    normed = rms_norm(dec_hidden, dec_gain)
    width = w_query.shape[0]
    rows = dec_hidden.shape[0]
    anywhere = pl.BlockSpec(memory_space=pl.ANY)
    dma = pltpu.SemaphoreType.DMA
    summed = pl.pallas_call(
        kernel,
        out_shape=jax.ShapeDtypeStruct((rows, width), BF16),
        in_specs=[pl.BlockSpec(memory_space=pltpu.SMEM)] + [anywhere] * 6,
        out_specs=pl.BlockSpec(memory_space=pltpu.VMEM),
        scratch_shapes=[
            pltpu.VMEM((NZ, 32, width), BF16),
            pltpu.VMEM((NZ, 128, width), BF16),
            pltpu.VMEM((2, 3, width, 256), BF16),
            pltpu.VMEM((2, 256, width), BF16),
            pltpu.VMEM((3, NZ, 2, 128, 256), BF16),
            pltpu.VMEM((3, 256, 256), BF16),
            pltpu.VMEM((4, 256, 512), BF16),
            pltpu.VMEM((256, 256), BF16),
            pltpu.VMEM((4, 64, 512), F32),
            pltpu.VMEM((4, 1, 512), F32),
            pltpu.VMEM((4, 1, 512), F32),
            pltpu.VMEM((3, 256, 256), BF16),
            pltpu.VMEM((256, width), F32),
            pltpu.VMEM((2, 7, 32, width // 2), BF16),
            pltpu.VMEM((2, 7, 32, width // 2), BF16),
            dma((6,)),
            dma((2, 18)),
            dma((2, 18)),
            dma((4,)),
            dma((4,)),
            dma((4,)),
            dma((4,)),
            dma((4, 2)),
            dma((4, 2)),
            dma((4,)),
            dma((4,)),
            dma((4,)),
            dma((NZ,)),
            dma((NZ,)),
            dma((2, 7)),
            dma((2, 7)),
        ],
        compiler_params=pltpu.CompilerParams(
            collective_id=0, has_side_effects=True, vmem_limit_bytes=60 * 1024 * 1024
        ),
        name="cross_attention",
    )(enc_length, normed, memory, w_query, w_key, w_value, w_out)
    row_ids = (lax.axis_index("yl") * NZ + lax.axis_index("z")) * rows + jnp.arange(rows, dtype=jnp.int32)
    cross_out = jnp.where((row_ids < dec_length[0])[:, None], summed, jnp.zeros_like(summed))
    return (memory, cross_out)


def solution(mesh):
    torus = Mesh(mesh.devices.reshape(4, 2, 2, 2, NZ), ROWS)
    tensor = ("yl", "z")
    dp = ("x", "yh", "c")
    in_specs = (
        P(ROWS, None),
        P(),
        P(ROWS, None),
        P(),
        P(None, tensor),
        P(None, tensor),
        P(None, tensor),
        P(tensor, None),
        P(dp),
        P(dp),
    )
    out_specs = (P(ROWS, None), P(ROWS, None))
    return jax.shard_map(shards, mesh=torus, in_specs=in_specs, out_specs=out_specs, check_vma=False)
```

```python
import functools

import jax
import jax.numpy as jnp
from jax import lax
from jax.experimental import pallas as pl
from jax.experimental.pallas import tpu as pltpu
from jax.sharding import Mesh
from jax.sharding import PartitionSpec as P

HEAD_DIM = 64
MESH = pl.DeviceIdType.MESH
NZ = 8
NEG = -1e30
ROWS = ("x", "yh", "c", "yl", "z")
BF16, F32 = jnp.bfloat16, jnp.float32

R_ITEMS = (
    [("n", 0, 0), ("m", 0, 0), ("n", 1, 0), ("m", 0, 1), ("n", 2, 0), ("m", 0, 2), ("n", 3, 0), ("m", 0, 3)]
    + [("m", 1, p) for p in range(4)]
    + [("m", 2, p) for p in range(4)]
    + [("m", 3, p) for p in (0, 4)]
)
L_ITEMS = (
    [("n", 0, 0), ("m", 0, 0), ("n", 1, 0), ("m", 0, 1), ("n", 2, 0), ("m", 0, 2), ("m", 0, 3)]
    + [("m", 1, p) for p in range(4)]
    + [("m", 2, p) for p in range(4)]
    + [("m", 3, p) for p in (2, 3, 5)]
)


def schedule(items):
    after, last = {}, -1
    for i, (kind, hop, piece) in enumerate(items):
        need = items.index((kind, hop - 1, 1 if piece > 3 else piece)) if hop else -1
        last = max(last, need)
        after.setdefault(last, []).append(i)
    return after


def piece_rows(piece):
    return pl.ds(32 * piece, 32) if piece < 4 else pl.ds(32 + 16 * (piece - 4), 16)


def rms_norm(values, gain):
    wide = values.astype(F32)
    mean_sq = jnp.mean(wide * wide, axis=-1, keepdims=True)
    return (wide * lax.rsqrt(mean_sq + 1e-06) * gain).astype(BF16)


def kernel(
    enc_len_hbm, dec_len_hbm, enc_hbm, encg_hbm, dec_hbm, decg_hbm, wq_hbm, wk_hbm, wv_hbm, wo_hbm, mem_out, out_ref,
    enc_len, dec_len, raw, gain, gn, gm, w, wo, kva, kvb, q, qtm, acc, mx, sm, ctx, both_ctx, rs_send, rs_recv,
    loc, z_send, z_recv, wy_send, wy_recv, xa_send, xa_recv, xb_send, xb_recv, c_send, c_recv,
    q_sem, ctx_sem, kva_send, kva_recv, kvb_send, kvb_recv, rss, rsr,
):
    x, c = lax.axis_index("x"), lax.axis_index("c")
    y, z = lax.axis_index("yl"), lax.axis_index("z")
    yn, cn = 1 - y, 1 - c
    xa, xb = x + 1 - 2 * (x % 2), 3 - x
    right, left = (z + 1) % NZ, (z + NZ - 1) % NZ
    peers = ({"z": right}, {"z": left}, {"yl": yn}, {"x": xa}, {"x": xb}, {"c": cn})

    barrier = pltpu.get_barrier_semaphore()
    for peer in peers:
        pl.semaphore_signal(barrier, inc=1, device_id=peer, device_id_type=MESH)

    enters = [
        pltpu.make_async_copy(dec_hbm, raw.at[pl.ds(0, 32), :], loc.at[0]),
        pltpu.make_async_copy(decg_hbm, gain.at[0], loc.at[1]),
        pltpu.make_async_copy(enc_hbm, raw.at[pl.ds(32, 128), :], loc.at[2]),
        pltpu.make_async_copy(encg_hbm, gain.at[1], loc.at[3]),
    ]
    local = [
        pltpu.make_async_copy(wk_hbm, w.at[0, 0], loc.at[4]),
        pltpu.make_async_copy(wv_hbm, w.at[0, 1], loc.at[5]),
        pltpu.make_async_copy(wq_hbm, w.at[0, 2], loc.at[6]),
        pltpu.make_async_copy(wo_hbm, wo.at[0], loc.at[7]),
        pltpu.make_async_copy(enc_len_hbm, enc_len, loc.at[9]),
        pltpu.make_async_copy(dec_len_hbm, dec_len, loc.at[10]),
    ]
    for copy in enters + local:
        copy.start()
    enters[0].wait()
    enters[1].wait()
    gn[z] = rms_norm(raw[pl.ds(0, 32), :], gain[0])
    enters[2].wait()
    enters[3].wait()

    def norm_piece(p):
        gm[z, pl.ds(32 * p, 32), :] = rms_norm(raw[pl.ds(32 + 32 * p, 32), :], gain[1])

    norm_piece(0)
    pl.semaphore_wait(barrier, len(peers))

    def remote(src, dst, ssem, rsem, peer):
        return pltpu.make_async_remote_copy(
            src_ref=src, dst_ref=dst, send_sem=ssem, recv_sem=rsem, device_id=peer, device_id_type=MESH
        )

    def z_ref(kind, owner, piece):
        return gn.at[owner] if kind == "n" else gm.at[owner, piece_rows(piece), :]

    def z_copy(d, i, receive):
        kind, hop, piece = (R_ITEMS, L_ITEMS)[d][i]
        shift = hop + (1 if receive else 0)
        owner = (z + (NZ - shift if d == 0 else shift)) % NZ
        block = z_ref(kind, owner, piece)
        return remote(block, block, z_send.at[d, i], z_recv.at[d, i], peers[d])

    plan = (schedule(R_ITEMS), schedule(L_ITEMS))

    def z_issue(d, k):
        for i in plan[d].get(k, ()):
            z_copy(d, i, False).start()

    def serve(d, k):
        z_copy(d, k, True).wait_recv()
        z_issue(d, k)

    hbm = (wk_hbm, wv_hbm, wq_hbm, wo_hbm)
    STEP = (512, 512, 512, 32)

    def part(t, e, n=1):
        rows = pl.ds(e * STEP[t], n * STEP[t])
        return wo.at[1, rows, :] if t == 3 else w.at[1, t, rows, :]

    mine = c * 4 + x

    def wy(t):
        src = hbm[t].at[pl.ds(mine * STEP[t], STEP[t]), :]
        return remote(src, part(t, mine), wy_send.at[t], wy_recv.at[t], peers[2])

    def wxa(t, receive=False):
        r = part(t, c * 4 + (xa if receive else x))
        return remote(r, r, xa_send.at[t], xa_recv.at[t], peers[3])

    def wxb(t, k, receive=False):
        near, far = (xb, xb + 1 - 2 * (xb % 2)) if receive else (x, xa)
        r = part(t, c * 4 + (far if k else near))
        return remote(r, r, xb_send.at[t, k], xb_recv.at[t, k], peers[4])

    def wc(t, receive=False):
        r = part(t, 4 * (cn if receive else c), 4)
        return remote(r, r, c_send.at[t], c_recv.at[t], peers[5])

    def got_y(t):
        wy(t).wait_recv()
        wxb(t, 0).start()
        wxa(t).start()

    def got_xa(t):
        wxa(t, True).wait_recv()
        wxb(t, 1).start()

    def got_xb(t):
        wxb(t, 0, True).wait_recv()
        wxb(t, 1, True).wait_recv()
        wc(t).start()

    for d in (0, 1):
        z_issue(d, -1)
    for t in range(4):
        wy(t).start()
    @pl.loop(1, 4)
    def _(p):
        norm_piece(p)

    mem_out[...] = gm[z]
    mx[...] = jnp.full_like(mx, NEG)
    sm[...] = jnp.zeros_like(sm)
    acc[...] = jnp.zeros_like(acc)

    def both(k):
        serve(0, k)
        serve(1, k)

    both(0)
    got_y(0)
    got_y(1)
    got_xa(0)
    both(1)
    got_y(2)
    got_xa(1)
    both(2)
    got_y(3)
    got_xa(2)
    got_xb(0)
    both(3)
    got_xb(1)
    got_xa(3)
    both(4)
    both(5)
    got_xb(2)
    both(6)
    serve(0, 7)
    for copy in local:
        copy.wait()
    for t in (2, 0, 1):
        wc(t, True).wait_recv()

    q_copy = remote(q.at[2], q.at[1], q_sem.at[0], q_sem.at[1], peers[2])
    tokens = gn[...].reshape(NZ * 32, gn.shape[2])

    @pl.loop(0, 2)
    def _(i):
        q[2 - 2 * i] = jnp.dot(tokens, w[1 - i, 2], preferred_element_type=F32).astype(BF16)

    q_copy.start()

    length = enc_len[0]

    def kv_copy(units, u):
        kv, ssem, rsem = ((kva, kva_send, kva_recv), (kvb, kvb_send, kvb_recv))[units]
        return remote(kv.at[2, u], kv.at[1, u], ssem.at[u], rsem.at[u], peers[2])

    def project(units, u, rows):
        kv = (kva, kvb)[units]
        for side in (2, 0):

            @pl.loop(0, 2)
            def _(which):
                kv[side, u, which] = jnp.dot(
                    rows, w[side // 2, which], preferred_element_type=F32
                ).astype(BF16)

            if side == 2:
                kv_copy(units, u).start()

    def attend(units, u, parts, last=False):
        kv = (kva, kvb)[units]
        n = 2 * kv.shape[3]
        kv_copy(units, u).wait_recv()
        keys = jnp.concatenate([kv[0, u, 0], kv[1, u, 0]], axis=0)
        values = jnp.concatenate([kv[0, u, 1], kv[1, u, 1]], axis=0)
        values_t = values.T
        index = []
        for row in (y, yn):
            for start, size in parts:
                index.append(lax.broadcasted_iota(jnp.int32, (size, 1), 0) + (row * NZ * 128 + start))
        valid = jnp.broadcast_to(jnp.concatenate(index, axis=0), (n, 512)) < length

        def head(h, v_h):
            s = jnp.dot(keys, qtm[h], preferred_element_type=F32)
            s = jnp.where(valid, s, NEG)
            old = mx[h]
            new = jnp.maximum(old, jnp.max(s, axis=0, keepdims=True))
            p = jnp.exp(s - new)
            scale = jnp.exp(old - new)
            total = scale * sm[h] + jnp.sum(p, axis=0, keepdims=True)
            summed = scale * acc[h] + jnp.dot(v_h, p.astype(BF16), preferred_element_type=F32)
            if last:
                return (summed * (1.0 / total)).astype(BF16)
            mx[h] = new
            sm[h] = total
            acc[h] = summed

        heads = [lambda h=h: head(h, values_t[64 * h : 64 * h + 64]) for h in range(4)]
        if last:
            return heads
        for run in heads:
            run()

    def pieces_of(units, u):
        if units:
            return [((z + 4) % NZ, u), ((z + 4) % NZ, u + 2)]
        late, near = u // 5, (u + 1) // 2
        block = (z + NZ + near - 2 * near * (u % 2)) % NZ
        sides = ((z + NZ - 3) % NZ, (z + 3) % NZ)
        return [
            ((1 - late) * block + late * sides[i // 2], (1 - late) * i + late * (2 * (u - 5) + i % 2))
            for i in range(4)
        ]

    def rows_of(units, u):
        parts = [
            gm[block, pl.ds(pl.multiple_of(32 * piece, 32), 32), :] for block, piece in pieces_of(units, u)
        ]
        return jnp.concatenate(parts, axis=0)

    def attend_unit(units, u, last=False):
        return attend(units, u, [(block * 128 + 32 * piece, 32) for block, piece in pieces_of(units, u)], last)

    before = {
        1: [(1, 7), (0, 8)],
        2: [(1, 8), (0, 9)],
        3: [(1, 9), (0, 10), (1, 10), (0, 11)],
        5: [(1, 11), (0, 12), (1, 12), (0, 13)],
        6: [(1, 13), (0, 14), (1, 14), (0, 15)],
    }

    @pl.loop(0, 7)
    def _(u):
        for at, todo in before.items():

            @pl.when(u == at)
            def _():
                for d, k in todo:
                    serve(d, k)

        @pl.when(u == 4)
        def _():
            got_xb(3)

        project(0, u, rows_of(0, u))

        @pl.when(u == 0)
        def _():
            q_copy.wait_recv()
            first = jnp.where(y == 0, q[0], q[1])
            second = jnp.where(y == 0, q[1], q[0])
            qt = jnp.concatenate([first.T, second.T], axis=1)
            column = lax.broadcasted_iota(jnp.int32, (256, 512), 0)
            for h in range(4):
                qtm[h] = jnp.where(column // HEAD_DIM == h, qt, jnp.zeros_like(qt))

        @pl.when(u > 0)
        def _():
            attend_unit(0, u - 1)

    serve(1, 15)
    serve(0, 16)
    project(1, 0, rows_of(1, 0))
    attend_unit(0, 6)
    serve(1, 16)
    serve(0, 17)
    serve(1, 17)
    project(1, 1, rows_of(1, 1))
    attend_unit(1, 0)

    heads = attend_unit(1, 1, True)

    def ctx_copy(pair):
        return remote(ctx.at[2, pair], ctx.at[1, pair], ctx_sem.at[0, pair], ctx_sem.at[1, pair], peers[2])

    for pair in (0, 1):
        full = jnp.concatenate([heads[2 * pair](), heads[2 * pair + 1]()], axis=0)
        low, high = full[:, :256].T, full[:, 256:].T
        ctx[2, pair] = jnp.where(y == 0, high, low)
        ctx_copy(pair).start()
        both_ctx[:, pl.ds(128 * pair, 128)] = jnp.where(y == 0, low, high)
    wc(3, True).wait_recv()
    for pair in (0, 1):
        ctx_copy(pair).wait_recv()
        both_ctx[:, pl.ds(256 + 128 * pair, 128)] = ctx[1, pair]

    orders = (
        [(0, 4), (1, 3), (0, 3), (1, 2), (0, 2), (1, 1), (0, 1)],
        [(1, 4), (0, 3), (1, 3), (0, 2), (1, 2), (0, 1), (1, 1)],
    )

    def rs_copy(d, i):
        return remote(rs_send.at[d, i], rs_recv.at[d, i], rss.at[d, i], rsr.at[d, i], peers[d])

    def term_of(owner, half):
        rows = both_ctx[pl.ds(pl.multiple_of(owner * 32, 32), 32), :]
        cols = pl.ds(half * 2048, 2048)
        return jnp.dot(rows[:, :256], wo[0, :, cols], preferred_element_type=F32) + jnp.dot(
            rows[:, 256:], wo[1, :, cols], preferred_element_type=F32
        )

    for i in range(7):
        for d in (0, 1):
            half, far = orders[d][i]
            term = term_of((z + (far if d == 0 else NZ - far)) % NZ, half)
            if i >= 2:
                rs_copy(d, i - 2).wait_recv()
                term = term + rs_recv[d, i - 2].astype(F32)
            rs_send[d, i] = term.astype(BF16)
            rs_copy(d, i).start()
    terms = [term_of(z, half) for half in (0, 1)]
    for d in (0, 1):
        for i in (5, 6):
            rs_copy(d, i).wait_recv()
    live = lax.broadcasted_iota(jnp.int32, (32, 2048), 0) + (y * NZ + z) * 32 < dec_len[0]
    for half in (0, 1):
        total = terms[half] + rs_recv[0, 6 - half].astype(F32) + rs_recv[1, 5 + half].astype(F32)
        out_ref[:, pl.ds(half * 2048, 2048)] = jnp.where(live, total, 0.0).astype(BF16)

    for d in (0, 1):
        for i in range(len((R_ITEMS, L_ITEMS)[d])):
            z_copy(d, i, False).wait_send()
        for i in range(7):
            rs_copy(d, i).wait_send()
    for t in range(4):
        wy(t).wait_send()
        wxa(t).wait_send()
        wxb(t, 0).wait_send()
        wxb(t, 1).wait_send()
        wc(t).wait_send()
    q_copy.wait_send()
    for pair in (0, 1):
        ctx_copy(pair).wait_send()
    for u in range(7):
        kv_copy(0, u).wait_send()
    for u in range(2):
        kv_copy(1, u).wait_send()


def shards(enc_hidden, enc_gain, dec_hidden, dec_gain, w_query, w_key, w_value, w_out, enc_length, dec_length):
    width = w_query.shape[0]
    rows = dec_hidden.shape[0]
    anywhere = pl.BlockSpec(memory_space=pl.ANY)
    dma = pltpu.SemaphoreType.DMA
    return pl.pallas_call(
        kernel,
        out_shape=(
            pltpu.VMEM(enc_hidden.shape, BF16),
            pltpu.VMEM((rows, width), BF16),
        ),
        in_specs=[anywhere] * 10,
        out_specs=(pl.BlockSpec(memory_space=pltpu.VMEM), pl.BlockSpec(memory_space=pltpu.VMEM)),
        scratch_shapes=[
            pltpu.SMEM((1,), jnp.int32),
            pltpu.SMEM((1,), jnp.int32),
            pltpu.VMEM((160, width), BF16),
            pltpu.VMEM((2, 1, width), F32),
            pltpu.VMEM((NZ, 32, width), BF16),
            pltpu.VMEM((NZ, 128, width), BF16),
            pltpu.VMEM((2, 3, width, 256), BF16),
            pltpu.VMEM((2, 256, width), BF16),
            pltpu.VMEM((3, 7, 2, 128, 256), BF16),
            pltpu.VMEM((3, 2, 2, 64, 256), BF16),
            pltpu.VMEM((3, 256, 256), BF16),
            pltpu.VMEM((4, 256, 512), BF16),
            pltpu.VMEM((4, 64, 512), F32),
            pltpu.VMEM((4, 1, 512), F32),
            pltpu.VMEM((4, 1, 512), F32),
            pltpu.VMEM((3, 2, 256, 128), BF16),
            pltpu.VMEM((256, 512), BF16),
            pltpu.VMEM((2, 7, 32, width // 2), BF16),
            pltpu.VMEM((2, 7, 32, width // 2), BF16),
            dma((11,)),
            dma((2, 18)),
            dma((2, 18)),
            dma((4,)),
            dma((4,)),
            dma((4,)),
            dma((4,)),
            dma((4, 2)),
            dma((4, 2)),
            dma((4,)),
            dma((4,)),
            dma((2,)),
            dma((2, 2)),
            dma((7,)),
            dma((7,)),
            dma((2,)),
            dma((2,)),
            dma((2, 7)),
            dma((2, 7)),
        ],
        compiler_params=pltpu.CompilerParams(
            collective_id=0, has_side_effects=True, vmem_limit_bytes=60 * 1024 * 1024
        ),
        name="cross_attention",
    )(
        enc_length,
        dec_length,
        enc_hidden,
        enc_gain.reshape(1, width),
        dec_hidden,
        dec_gain.reshape(1, width),
        w_query,
        w_key,
        w_value,
        w_out,
    )


def solution(mesh):
    torus = Mesh(mesh.devices.reshape(4, 2, 2, 2, NZ), ROWS)
    tensor = ("yl", "z")
    dp = ("x", "yh", "c")
    in_specs = (
        P(ROWS, None),
        P(),
        P(ROWS, None),
        P(),
        P(None, tensor),
        P(None, tensor),
        P(None, tensor),
        P(tensor, None),
        P(dp),
        P(dp),
    )
    out_specs = (P(ROWS, None), P(ROWS, None))
    return jax.shard_map(shards, mesh=torus, in_specs=in_specs, out_specs=out_specs, check_vma=False)
```

```python
import functools

import jax
import jax.numpy as jnp
from jax import lax
from jax.experimental import pallas as pl
from jax.experimental.pallas import tpu as pltpu
from jax.sharding import Mesh
from jax.sharding import PartitionSpec as P

HEAD_DIM = 64
MESH = pl.DeviceIdType.MESH
NZ = 8
NEG = -1e30
ROWS = ("x", "yh", "c", "yl", "z")
BF16, F32 = jnp.bfloat16, jnp.float32

OUTER = (
    [("n", 0, 0), ("m", 0, 0), ("n", 1, 0), ("m", 0, 1), ("n", 2, 0), ("m", 0, 2), ("n", 3, 4), ("m", 0, 3)]
    + [("m", 1, p) for p in range(4)]
    + [("m", 2, p) for p in range(4)]
)
INNER = (
    [("n", 0, 0), ("w", 0, 0), ("n", 1, 0), ("w", 0, 1), ("n", 2, 0), ("m", 0, 0), ("n", 3, 5)]
    + [("m", 0, p) for p in (1, 2, 3)]
    + [("m", 1, p) for p in range(4)]
)
ITEMS = (OUTER, INNER)


def schedule(d):
    after, last = {}, -1
    for i, (kind, hop, piece) in enumerate(ITEMS[d]):
        if hop:
            last = max(last, ITEMS[1 - d].index((kind, hop - 1, piece % 4 if kind == "m" else 0)))
        after.setdefault(last, []).append(i)
    return after


def rms_norm(values, gain):
    wide = values.astype(F32)
    mean_sq = jnp.mean(wide * wide, axis=-1, keepdims=True)
    return (wide * lax.rsqrt(mean_sq + 1e-06) * gain).astype(BF16)


def kernel(
    enc_len_hbm, dec_len_hbm, enc_hbm, encg_hbm, dec_hbm, decg_hbm, wq_hbm, wk_hbm, wv_hbm, wo_hbm, mem_out, out_ref,
    enc_len, dec_len, raw, gain, gn, gm, w, w2, wo, kva, kvb, kvc, q, qtm, acc, mx, sm, ctx, both_ctx, rs_send, rs_recv,
    ready, loc, z_send, z_recv, wy_send, wy_recv, xa_send, xa_recv, xb_send, xb_recv, c_send, c_recv,
    q_sem, ctx_sem, kva_send, kva_recv, kvb_send, kvb_recv, kvc_send, kvc_recv, as_send, as_recv, rss, rsr,
):
    x, c = lax.axis_index("x"), lax.axis_index("c")
    y, z = lax.axis_index("yl"), lax.axis_index("z")
    yh = lax.axis_index("yh")
    yn, cn = 1 - y, 1 - c
    xa, xb = x + 1 - 2 * (x % 2), 3 - x
    right, left = (z + 1) % NZ, (z + NZ - 1) % NZ
    sign = 1 - 2 * (z % 2)
    inner, outer = z + sign, (z + NZ - sign) % NZ
    ring = ({"z": right}, {"z": left})
    peers = ({"z": outer}, {"z": inner}, {"yl": yn}, {"x": xa}, {"x": xb}, {"c": cn}, {"yl": yn, "z": inner})
    peers += ({"yl": yn, "yh": 1 - yh},)

    barrier = pltpu.get_barrier_semaphore()

    def greet(*to):
        for peer in to:
            pl.semaphore_signal(barrier, inc=1, device_id=peer, device_id_type=MESH)

    def answer(which, peer):
        pl.semaphore_signal(ready.at[which], inc=1, device_id=peer, device_id_type=MESH)

    greet(*peers[:3], *peers[6:])
    pl.when(c == 0)(lambda: greet(peers[5]))
    pl.when(x == 0)(lambda: greet(peers[3], peers[4]))
    pl.when(x == 1)(lambda: greet(peers[4]))
    pl.when(x == 3)(lambda: greet(peers[3]))

    enters = [
        pltpu.make_async_copy(dec_hbm, raw.at[pl.ds(0, 32), :], loc.at[0]),
        pltpu.make_async_copy(decg_hbm, gain.at[0], loc.at[1]),
        pltpu.make_async_copy(enc_hbm, raw.at[pl.ds(32, 128), :], loc.at[2]),
        pltpu.make_async_copy(encg_hbm, gain.at[1], loc.at[3]),
    ]
    local = [
        pltpu.make_async_copy(wk_hbm, w.at[0, 0], loc.at[4]),
        pltpu.make_async_copy(wv_hbm, w.at[0, 1], loc.at[5]),
        pltpu.make_async_copy(wq_hbm, w.at[0, 2], loc.at[6]),
        pltpu.make_async_copy(wo_hbm, wo.at[0], loc.at[7]),
        pltpu.make_async_copy(enc_len_hbm, enc_len, loc.at[9]),
        pltpu.make_async_copy(dec_len_hbm, dec_len, loc.at[10]),
    ]
    for copy in enters + local:
        copy.start()
    enters[0].wait()
    enters[1].wait()
    gn[z] = rms_norm(raw[pl.ds(0, 32), :], gain[0])
    enters[2].wait()
    enters[3].wait()

    def norm_piece(p):
        gm[z, pl.ds(32 * p, 32), :] = rms_norm(raw[pl.ds(32 + 32 * p, 32), :], gain[1])

    norm_piece(0)
    pl.semaphore_wait(barrier, 5 + c + x - 2 * (x // 3))

    def remote(src, dst, ssem, rsem, peer):
        return pltpu.make_async_remote_copy(
            src_ref=src, dst_ref=dst, send_sem=ssem, recv_sem=rsem, device_id=peer, device_id_type=MESH
        )

    hbm = (wk_hbm, wv_hbm, wq_hbm, wo_hbm)

    def partner_of(t, at):
        return at + 1 - 2 * (at % 2) if t in (1, 3, 4, 6) else 3 - at

    def held(t, at, other=False):
        flip = 1 - yh if other else yh
        return c * 4 + at + flip * (partner_of(t, at) - at)


    def part(t, e, n=1):
        if t == 3:
            return wo.at[1, pl.ds(e * 32, n * 32), :]
        rows = pl.ds(e * 512, n * 512)
        return w.at[1, t, rows, :] if t < 3 else w2.at[t // 2 - 2, t % 2, rows, :]

    def z_ref(kind, owner, piece):
        if kind == "n":
            return gn.at[owner] if piece == 0 else gn.at[owner, pl.ds(16 * (piece - 4), 16), :]
        return gm.at[owner, pl.ds(32 * piece, 32), :]

    def z_copy(d, i, receive):
        kind, hop, piece = ITEMS[d][i]
        if kind == "w":
            e = held(4 + piece, x)
            src, dst = hbm[piece].at[pl.ds(e * 512, 512), :], part(4 + piece, e)
        else:
            away = sign if d == (1 if receive else 0) else -sign
            src = dst = z_ref(kind, (z + NZ + away * (hop + (1 if receive else 0))) % NZ, piece)
        return remote(src, dst, z_send.at[d, i], z_recv.at[d, i], peers[d])

    plan = (schedule(0), schedule(1))

    def z_issue(d, k):
        for i in plan[d].get(k, ()):
            z_copy(d, i, False).start()

    def serve(d, k):
        z_copy(d, k, True).wait_recv()
        z_issue(1 - d, k)

    def wy(t, far, receive=False):
        e = held(t, x, receive and far == 1)
        size = 32 if t == 3 else 512
        src = hbm[t].at[pl.ds(e * size, size), :] if t < 4 else part(t - 2, e)
        return remote(src, part(t, e), wy_send.at[t, far], wy_recv.at[t, far], peers[7 if far else 2])

    def wx(t, k, receive=False):
        if t in (4, 5):
            near, at, peer = ((xa, xb, 4), (xb, xa, 3))[t - 4]
            e = held(t, (3 - xa if k else at) if receive else (near if k else x))
        else:
            at, peer = (xb, 4) if t in (1, 3, 6) else (xa, 3)
            e = held(t, at if receive else x, k == 1)
        return remote(part(t, e), part(t, e), xb_send.at[t, k], xb_recv.at[t, k], peers[peer])

    def wnear(t, receive=False):
        at, peer = ((xa, 3), (xb, 4))[t - 4]
        r = part(t, held(t, at if receive else x))
        return remote(r, r, xa_send.at[t], xa_recv.at[t], peers[peer])

    def wc(t, receive=False):
        r = part(t, 4 * (cn if receive else c), 4)
        return remote(r, r, c_send.at[t], c_recv.at[t], peers[5])

    def send_y(t):
        wy(t, 0).start()
        wy(t, 1).start()

    def got_y(t):
        for k in (0, 1):
            wy(t, k, True).wait_recv()
        for k in (0, 1):
            wx(t, k).start()

    def got_z(t):
        send_y(t + 2)
        wx(t, 0).start()
        wnear(t).start()

    def got_near(t):
        wnear(t, True).wait_recv()
        wx(t, 1).start()

    def got_x(t):
        for k in (0, 1):
            wx(t, k, True).wait_recv()
        wc(t).start()

    for d in (0, 1):
        z_issue(d, -1)
    for t in range(3):
        send_y(t)
    pl.when(c == 1)(lambda: answer(0, peers[5]))
    pl.when(x == 1)(lambda: answer(1, peers[3]))
    pl.when(x == 3)(lambda: answer(2, peers[4]))

    @pl.when(x == 2)
    def _():
        answer(1, peers[3])
        answer(2, peers[4])
    @pl.loop(1, 4)
    def _(p):
        norm_piece(p)

    mem_out[...] = gm[z]
    mx[...] = jnp.full_like(mx, NEG)
    sm[...] = jnp.zeros_like(sm)
    acc[...] = jnp.zeros_like(acc)

    def both(k):
        serve(0, k)
        serve(1, k)

    both(0)

    @pl.when(x // 2 == 0)
    def _():
        pl.semaphore_wait(ready.at[2], 1)

    pl.when(x % 3 == 0)(lambda: pl.semaphore_wait(ready.at[1], 1))
    got_y(0)
    got_y(1)
    both(1)
    got_z(4)
    got_y(2)
    both(2)
    both(3)
    got_z(5)
    send_y(3)
    got_y(6)
    pl.when(c == 0)(lambda: pl.semaphore_wait(ready.at[0], 1))
    got_x(0)
    got_near(4)
    both(4)
    got_x(1)
    got_y(7)
    both(5)
    got_x(2)
    both(6)
    serve(0, 7)
    for copy in local:
        copy.wait()
    for t in (2, 0, 1):
        wc(t, True).wait_recv()

    q_copy = remote(q.at[2], q.at[1], q_sem.at[0], q_sem.at[1], peers[2])
    tokens = gn[...].reshape(NZ * 32, gn.shape[2])

    @pl.loop(0, 2)
    def _(i):
        q[2 - 2 * i] = jnp.dot(tokens, w[1 - i, 2], preferred_element_type=F32).astype(BF16)

    q_copy.start()

    length = enc_len[0]

    kvs, seen = (kva, kvb, kvc), (5, 1, 1)
    kv_sems = ((kva_send, kva_recv), (kvb_send, kvb_recv), (kvc_send, kvc_recv))

    def kv_copy(units, u):
        kv, (ssem, rsem) = kvs[units], kv_sems[units]
        return remote(kv.at[2, u], kv.at[1, u], ssem.at[u], rsem.at[u], peers[2])

    def help_copy(units, side):
        kv, there = kvs[units], seen[units]
        return remote(
            kv.at[side, there + 1],
            kv.at[side, there],
            as_send.at[units, side],
            as_recv.at[units, side],
            peers[6 if side else 1],
        )

    def project(units, u, rows, sides=(2, 0)):
        kv = kvs[units]
        for side in sides:

            @pl.loop(0, 2)
            def _(which):
                kv[side, u, which] = jnp.dot(
                    rows, w[side // 2, which], preferred_element_type=F32
                ).astype(BF16)

            if side == 2:
                kv_copy(units, u).start()

    def assist(units, rows):
        kv, here = kvs[units], seen[units] + 1
        for side in (1, 0):

            @pl.loop(0, 2)
            def _(which):
                kv[side, here, which] = jnp.dot(rows, w2[side, which], preferred_element_type=F32).astype(BF16)

            help_copy(units, side).start()

    def attend(slots, last=False):
        keys, values, index = [], [], []
        for units, u, block, start in slots:
            kv = kvs[units]
            if not isinstance(u, int) or u < seen[units]:
                kv_copy(units, u).wait_recv()
            else:
                help_copy(units, 0).wait_recv()
                help_copy(units, 1).wait_recv()
            for side, row in ((0, y), (1, yn)):
                size = kv.shape[3]
                keys.append(kv[side, u, 0])
                values.append(kv[side, u, 1])
                base = (row * NZ + block) * 128 + start
                index.append(lax.broadcasted_iota(jnp.int32, (size, 1), 0) + base)
        keys = jnp.concatenate(keys, axis=0)
        values_t = jnp.concatenate(values, axis=0).T
        valid = jnp.broadcast_to(jnp.concatenate(index, axis=0), (keys.shape[0], 512)) < length

        def head(h, v_h):
            s = jnp.dot(keys, qtm[h], preferred_element_type=F32)
            s = jnp.where(valid, s, NEG)
            old = mx[h]
            new = jnp.maximum(old, jnp.max(s, axis=0, keepdims=True))
            p = jnp.exp(s - new)
            scale = jnp.exp(old - new)
            total = scale * sm[h] + jnp.sum(p, axis=0, keepdims=True)
            summed = scale * acc[h] + jnp.dot(v_h, p.astype(BF16), preferred_element_type=F32)
            if last:
                return (summed * (1.0 / total)).astype(BF16)
            mx[h] = new
            sm[h] = total
            acc[h] = summed

        heads = [lambda h=h: head(h, values_t[64 * h : 64 * h + 64]) for h in range(4)]
        if last:
            return heads
        for run in heads:
            run()

    def block_of(u):
        return (z + NZ + sign * ((u + 1) // 2) * (1 - 2 * (u % 2))) % NZ

    ends = {1: (0, 96), 2: (96, 32)}

    def end_rows(units):
        return gm[(z + NZ - 3 * sign) % NZ, pl.ds(*ends[units]), :]

    def end_slots(units):
        start = ends[units][0]
        return [(units, 0, (z + NZ - 3 * sign) % NZ, start), (units, 1, (z + 4) % NZ, start)]

    before = {
        1: lambda: (serve(1, 7), got_near(5), got_y(3)),
        2: lambda: (serve(1, 8), serve(0, 8), got_x(6), got_x(4), serve(1, 9), serve(0, 9)),
        3: lambda: (serve(0, 10), serve(1, 10), got_x(7), got_x(5), serve(0, 11), serve(1, 11)),
    }

    @pl.loop(0, 4)
    def _(u):
        for at, take in before.items():

            @pl.when(u == at)
            def _():
                take()

        project(0, u, gm[block_of(u)])

        @pl.when(u == 0)
        def _():
            q_copy.wait_recv()
            first = jnp.where(y == 0, q[0], q[1])
            second = jnp.where(y == 0, q[1], q[0])
            qt = jnp.concatenate([first.T, second.T], axis=1)
            column = lax.broadcasted_iota(jnp.int32, (256, 512), 0)
            for h in range(4):
                qtm[h] = jnp.where(column // HEAD_DIM == h, qt, jnp.zeros_like(qt))

        attend([(0, u, block_of(u), 0)])

    serve(1, 12)
    serve(0, 12)
    for t in (4, 5, 6, 7):
        wc(t, True).wait_recv()
    assist(0, gm[block_of(3)])
    serve(1, 13)
    serve(0, 13)
    got_x(3)
    project(0, 4, gm[block_of(4)])
    attend([(0, 5, (z + NZ + 3 * sign) % NZ, 0)])
    attend([(0, 4, block_of(4), 0)])
    serve(0, 14)
    rows = end_rows(1)
    assist(1, rows)
    project(1, 0, rows)
    serve(0, 15)
    rows = end_rows(2)
    assist(2, rows)
    project(2, 0, rows, (2,))
    attend(end_slots(1))
    project(2, 0, rows, (0,))

    heads = attend(end_slots(2), True)

    def ctx_copy(pair):
        return remote(ctx.at[2, pair], ctx.at[1, pair], ctx_sem.at[0, pair], ctx_sem.at[1, pair], peers[2])

    for pair in (0, 1):
        full = jnp.concatenate([heads[2 * pair](), heads[2 * pair + 1]()], axis=0)
        low, high = full[:, :256].T, full[:, 256:].T
        ctx[2, pair] = jnp.where(y == 0, high, low)
        ctx_copy(pair).start()
        both_ctx[:, pl.ds(128 * pair, 128)] = jnp.where(y == 0, low, high)
    wc(3, True).wait_recv()
    for pair in (0, 1):
        ctx_copy(pair).wait_recv()
        both_ctx[:, pl.ds(256 + 128 * pair, 128)] = ctx[1, pair]

    orders = []
    for long in ((0, 1), (2, 3)):
        short = (2, 3) if long[0] == 0 else (0, 1)
        order = [(quarter, 4) for quarter in long]
        for far in (3, 2, 1):
            order += [(quarter, far) for quarter in short + long]
        orders.append(order)
    n_rs = len(orders[0])

    def rs_copy(d, i):
        return remote(rs_send.at[d, i], rs_recv.at[d, i], rss.at[d, i], rsr.at[d, i], ring[d])

    def term_of(owner, quarter):
        rows = both_ctx[pl.ds(pl.multiple_of(owner * 32, 32), 32), :]
        cols = pl.ds(quarter * 1024, 1024)
        return jnp.dot(rows[:, :256], wo[0, :, cols], preferred_element_type=F32) + jnp.dot(
            rows[:, 256:], wo[1, :, cols], preferred_element_type=F32
        )

    for i in range(n_rs):
        for d in (0, 1):
            quarter, far = orders[d][i]
            term = term_of((z + (far if d == 0 else NZ - far)) % NZ, quarter)
            if (quarter, far + 1) in orders[d]:
                k = orders[d].index((quarter, far + 1))
                rs_copy(d, k).wait_recv()
                term = term + rs_recv[d, k].astype(F32)
            rs_send[d, i] = term.astype(BF16)
            rs_copy(d, i).start()
    terms = [term_of(z, quarter) for quarter in range(4)]
    live = lax.broadcasted_iota(jnp.int32, (32, 1024), 0) + (y * NZ + z) * 32 < dec_len[0]
    for i in range(n_rs - 4, n_rs):
        for d in (0, 1):
            rs_copy(d, i).wait_recv()
            quarter = orders[d][i][0]
            terms[quarter] = terms[quarter] + rs_recv[d, i].astype(F32)
    for quarter in range(4):
        out_ref[:, pl.ds(quarter * 1024, 1024)] = jnp.where(live, terms[quarter], 0.0).astype(BF16)

    for d in (0, 1):
        for i in range(len(ITEMS[d])):
            z_copy(d, i, False).wait_send()
        for i in range(n_rs):
            rs_copy(d, i).wait_send()
    for t in range(8):
        for k in (0, 1):
            if t not in (4, 5):
                wy(t, k).wait_send()
            wx(t, k).wait_send()
        if t in (4, 5):
            wnear(t).wait_send()
        wc(t).wait_send()
    q_copy.wait_send()
    for pair in (0, 1):
        ctx_copy(pair).wait_send()
    for u in range(5):
        kv_copy(0, u).wait_send()
    for units in (1, 2):
        kv_copy(units, 0).wait_send()
    for units in range(3):
        for side in (0, 1):
            help_copy(units, side).wait_send()


def shards(enc_hidden, enc_gain, dec_hidden, dec_gain, w_query, w_key, w_value, w_out, enc_length, dec_length):
    width = w_query.shape[0]
    rows = dec_hidden.shape[0]
    anywhere = pl.BlockSpec(memory_space=pl.ANY)
    dma = pltpu.SemaphoreType.DMA
    return pl.pallas_call(
        kernel,
        out_shape=(
            pltpu.VMEM(enc_hidden.shape, BF16),
            pltpu.VMEM((rows, width), BF16),
        ),
        in_specs=[anywhere] * 10,
        out_specs=(pl.BlockSpec(memory_space=pltpu.VMEM), pl.BlockSpec(memory_space=pltpu.VMEM)),
        scratch_shapes=[
            pltpu.SMEM((1,), jnp.int32),
            pltpu.SMEM((1,), jnp.int32),
            pltpu.VMEM((160, width), BF16),
            pltpu.VMEM((2, 1, width), F32),
            pltpu.VMEM((NZ, 32, width), BF16),
            pltpu.VMEM((NZ, 128, width), BF16),
            pltpu.VMEM((2, 3, width, 256), BF16),
            pltpu.VMEM((2, 2, width, 256), BF16),
            pltpu.VMEM((2, 256, width), BF16),
            pltpu.VMEM((3, 7, 2, 128, 256), BF16),
            pltpu.VMEM((3, 3, 2, 96, 256), BF16),
            pltpu.VMEM((3, 3, 2, 32, 256), BF16),
            pltpu.VMEM((3, 256, 256), BF16),
            pltpu.VMEM((4, 256, 512), BF16),
            pltpu.VMEM((4, 64, 512), F32),
            pltpu.VMEM((4, 1, 512), F32),
            pltpu.VMEM((4, 1, 512), F32),
            pltpu.VMEM((3, 2, 256, 128), BF16),
            pltpu.VMEM((256, 512), BF16),
            pltpu.VMEM((2, 14, 32, width // 4), BF16),
            pltpu.VMEM((2, 14, 32, width // 4), BF16),
            pltpu.SemaphoreType.REGULAR((3,)),
            dma((11,)),
            dma((2, 16)),
            dma((2, 16)),
            dma((8, 2)),
            dma((8, 2)),
            dma((8,)),
            dma((8,)),
            dma((8, 2)),
            dma((8, 2)),
            dma((8,)),
            dma((8,)),
            dma((2,)),
            dma((2, 2)),
            dma((5,)),
            dma((5,)),
            dma((1,)),
            dma((1,)),
            dma((1,)),
            dma((1,)),
            dma((3, 2)),
            dma((3, 2)),
            dma((2, 14)),
            dma((2, 14)),
        ],
        compiler_params=pltpu.CompilerParams(
            collective_id=0, has_side_effects=True, vmem_limit_bytes=60 * 1024 * 1024
        ),
        name="cross_attention",
    )(
        enc_length,
        dec_length,
        enc_hidden,
        enc_gain.reshape(1, width),
        dec_hidden,
        dec_gain.reshape(1, width),
        w_query,
        w_key,
        w_value,
        w_out,
    )


def solution(mesh):
    torus = Mesh(mesh.devices.reshape(4, 2, 2, 2, NZ), ROWS)
    tensor = ("yl", "z")
    dp = ("x", "yh", "c")
    in_specs = (
        P(ROWS, None),
        P(),
        P(ROWS, None),
        P(),
        P(None, tensor),
        P(None, tensor),
        P(None, tensor),
        P(tensor, None),
        P(dp),
        P(dp),
    )
    out_specs = (P(ROWS, None), P(ROWS, None))
    return jax.shard_map(shards, mesh=torus, in_specs=in_specs, out_specs=out_specs, check_vma=False)
```

```python
import functools

import jax
import jax.numpy as jnp
from jax import lax
from jax.experimental import pallas as pl
from jax.experimental.pallas import tpu as pltpu
from jax.sharding import Mesh
from jax.sharding import PartitionSpec as P

HEAD_DIM = 64
MESH = pl.DeviceIdType.MESH
NZ = 8
NEG = -1e30
ROWS = ("x", "yh", "c", "yl", "z")
BF16, F32 = jnp.bfloat16, jnp.float32

OUTER = (
    [("n", 0, 0), ("m", 0, 0), ("n", 1, 0), ("m", 0, 1), ("n", 2, 0), ("m", 0, 2), ("n", 3, 4), ("m", 0, 3)]
    + [("m", 1, p) for p in range(4)]
    + [("m", 2, p) for p in range(4)]
)
INNER = (
    [("n", 0, 0), ("w", 0, 0), ("n", 1, 0), ("w", 0, 1), ("n", 2, 0), ("m", 0, 0), ("n", 3, 5)]
    + [("m", 0, p) for p in (1, 2, 3)]
    + [("m", 1, p) for p in range(4)]
)
ITEMS = (OUTER, INNER)


def schedule(d):
    after, last = {}, -1
    for i, (kind, hop, piece) in enumerate(ITEMS[d]):
        if hop:
            last = max(last, ITEMS[1 - d].index((kind, hop - 1, piece % 4 if kind == "m" else 0)))
        after.setdefault(last, []).append(i)
    return after


def rms_norm(values, gain):
    wide = values.astype(F32)
    mean_sq = jnp.mean(wide * wide, axis=-1, keepdims=True)
    return (wide * lax.rsqrt(mean_sq + 1e-06) * gain).astype(BF16)


def kernel(
    enc_len_hbm, dec_len_hbm, enc_hbm, encg_hbm, dec_hbm, decg_hbm, wq_hbm, wk_hbm, wv_hbm, wo_hbm, mem_out, out_ref,
    enc_len, dec_len, raw, gain, gn, gm, w, w2, wo, kva, kvb, kvc, q, qtm, acc, mx, sm, ctx, both_ctx, rs_send, rs_recv,
    ready, loc, z_send, z_recv, wy_send, wy_recv, xa_send, xa_recv, xb_send, xb_recv, c_send, c_recv,
    q_sem, ctx_sem, kva_send, kva_recv, kvb_send, kvb_recv, kvc_send, kvc_recv, as_send, as_recv, rss, rsr,
):
    x, c = lax.axis_index("x"), lax.axis_index("c")
    y, z = lax.axis_index("yl"), lax.axis_index("z")
    yh = lax.axis_index("yh")
    yn, cn = 1 - y, 1 - c
    xa, xb = x + 1 - 2 * (x % 2), 3 - x
    right, left = (z + 1) % NZ, (z + NZ - 1) % NZ
    sign = 1 - 2 * (z % 2)
    inner, outer = z + sign, (z + NZ - sign) % NZ
    ring = ({"z": right}, {"z": left})
    peers = ({"z": outer}, {"z": inner}, {"yl": yn}, {"x": xa}, {"x": xb}, {"c": cn}, {"yl": yn, "z": inner})
    peers += ({"yl": yn, "yh": 1 - yh},)

    barrier = pltpu.get_barrier_semaphore()

    def greet(*to):
        for peer in to:
            pl.semaphore_signal(barrier, inc=1, device_id=peer, device_id_type=MESH)

    def answer(which, peer):
        pl.semaphore_signal(ready.at[which], inc=1, device_id=peer, device_id_type=MESH)

    greet(*peers[:3], *peers[6:])
    pl.when(c == 0)(lambda: greet(peers[5]))
    pl.when(x == 0)(lambda: greet(peers[3], peers[4]))
    pl.when(x == 1)(lambda: greet(peers[4]))
    pl.when(x == 3)(lambda: greet(peers[3]))

    enters = [
        pltpu.make_async_copy(dec_hbm, raw.at[pl.ds(0, 32), :], loc.at[0]),
        pltpu.make_async_copy(decg_hbm, gain.at[0], loc.at[1]),
        pltpu.make_async_copy(enc_hbm, raw.at[pl.ds(32, 128), :], loc.at[2]),
        pltpu.make_async_copy(encg_hbm, gain.at[1], loc.at[3]),
    ]
    local = [
        pltpu.make_async_copy(wk_hbm, w.at[0, 0], loc.at[4]),
        pltpu.make_async_copy(wv_hbm, w.at[0, 1], loc.at[5]),
        pltpu.make_async_copy(wq_hbm, w.at[0, 2], loc.at[6]),
        pltpu.make_async_copy(wo_hbm, wo.at[0], loc.at[7]),
        pltpu.make_async_copy(enc_len_hbm, enc_len, loc.at[9]),
        pltpu.make_async_copy(dec_len_hbm, dec_len, loc.at[10]),
    ]
    for copy in enters + local:
        copy.start()
    enters[0].wait()
    enters[1].wait()
    gn[z] = rms_norm(raw[pl.ds(0, 32), :], gain[0])
    enters[2].wait()
    enters[3].wait()

    def norm_piece(p):
        gm[z, pl.ds(32 * p, 32), :] = rms_norm(raw[pl.ds(32 + 32 * p, 32), :], gain[1])

    norm_piece(0)
    pl.semaphore_wait(barrier, 5 + c + x - 2 * (x // 3))

    def remote(src, dst, ssem, rsem, peer):
        return pltpu.make_async_remote_copy(
            src_ref=src, dst_ref=dst, send_sem=ssem, recv_sem=rsem, device_id=peer, device_id_type=MESH
        )

    hbm = (wk_hbm, wv_hbm, wq_hbm, wo_hbm)

    def partner_of(t, at):
        return at + 1 - 2 * (at % 2) if t in (1, 3, 4, 6) else 3 - at

    def held(t, at, other=False):
        flip = 1 - yh if other else yh
        return c * 4 + at + flip * (partner_of(t, at) - at)


    def part(t, e, n=1):
        if t == 3:
            return wo.at[1, pl.ds(e * 32, n * 32), :]
        rows = pl.ds(e * 512, n * 512)
        return w.at[1, t, rows, :] if t < 3 else w2.at[t // 2 - 2, t % 2, rows, :]

    def z_ref(kind, owner, piece):
        if kind == "n":
            return gn.at[owner] if piece == 0 else gn.at[owner, pl.ds(16 * (piece - 4), 16), :]
        return gm.at[owner, pl.ds(32 * piece, 32), :]

    def z_copy(d, i, receive):
        kind, hop, piece = ITEMS[d][i]
        if kind == "w":
            e = held(4 + piece, x)
            src, dst = hbm[piece].at[pl.ds(e * 512, 512), :], part(4 + piece, e)
        else:
            away = sign if d == (1 if receive else 0) else -sign
            src = dst = z_ref(kind, (z + NZ + away * (hop + (1 if receive else 0))) % NZ, piece)
        return remote(src, dst, z_send.at[d, i], z_recv.at[d, i], peers[d])

    plan = (schedule(0), schedule(1))

    def z_issue(d, k):
        for i in plan[d].get(k, ()):
            z_copy(d, i, False).start()

    def serve(d, k):
        z_copy(d, k, True).wait_recv()
        z_issue(1 - d, k)

    def wy(t, far, receive=False):
        e = held(t, x, receive and far == 1)
        size = 32 if t == 3 else 512
        src = hbm[t].at[pl.ds(e * size, size), :] if t < 4 else part(t - 2, e)
        return remote(src, part(t, e), wy_send.at[t, far], wy_recv.at[t, far], peers[7 if far else 2])

    def wx(t, k, receive=False):
        if t in (4, 5):
            near, at, peer = ((xa, xb, 4), (xb, xa, 3))[t - 4]
            e = held(t, (3 - xa if k else at) if receive else (near if k else x))
        else:
            at, peer = (xb, 4) if t in (1, 3, 6) else (xa, 3)
            e = held(t, at if receive else x, k == 1)
        return remote(part(t, e), part(t, e), xb_send.at[t, k], xb_recv.at[t, k], peers[peer])

    def wnear(t, receive=False):
        at, peer = ((xa, 3), (xb, 4))[t - 4]
        r = part(t, held(t, at if receive else x))
        return remote(r, r, xa_send.at[t], xa_recv.at[t], peers[peer])

    def wc(t, receive=False):
        r = part(t, 4 * (cn if receive else c), 4)
        return remote(r, r, c_send.at[t], c_recv.at[t], peers[5])

    def send_y(t):
        wy(t, 0).start()
        wy(t, 1).start()

    def got_y(t):
        for k in (0, 1):
            wy(t, k, True).wait_recv()
        for k in (0, 1):
            wx(t, k).start()

    def got_z(t):
        send_y(t + 2)
        wx(t, 0).start()
        wnear(t).start()

    def got_near(t):
        wnear(t, True).wait_recv()
        wx(t, 1).start()

    def got_x(t):
        for k in (0, 1):
            wx(t, k, True).wait_recv()
        wc(t).start()

    for d in (0, 1):
        z_issue(d, -1)
    for t in range(3):
        send_y(t)
    pl.when(c == 1)(lambda: answer(0, peers[5]))
    pl.when(x == 1)(lambda: answer(1, peers[3]))
    pl.when(x == 3)(lambda: answer(2, peers[4]))

    @pl.when(x == 2)
    def _():
        answer(1, peers[3])
        answer(2, peers[4])
    @pl.loop(1, 4)
    def _(p):
        norm_piece(p)

    mem_out[...] = gm[z]
    mx[...] = jnp.full_like(mx, NEG)
    sm[...] = jnp.zeros_like(sm)
    acc[...] = jnp.zeros_like(acc)

    def both(k):
        serve(0, k)
        serve(1, k)

    both(0)

    @pl.when(x // 2 == 0)
    def _():
        pl.semaphore_wait(ready.at[2], 1)

    pl.when(x % 3 == 0)(lambda: pl.semaphore_wait(ready.at[1], 1))
    got_y(0)
    got_y(1)
    both(1)
    got_z(4)
    got_y(2)
    both(2)
    both(3)
    got_z(5)
    send_y(3)
    got_y(6)
    pl.when(c == 0)(lambda: pl.semaphore_wait(ready.at[0], 1))
    got_x(0)
    got_near(4)
    both(4)
    got_x(1)
    got_y(7)
    both(5)
    got_x(2)
    both(6)
    got_near(5)
    serve(0, 7)
    for copy in local:
        copy.wait()
    for t in (2, 0, 1):
        wc(t, True).wait_recv()

    q_copy = remote(q.at[2], q.at[1], q_sem.at[0], q_sem.at[1], peers[2])
    tokens = gn[...].reshape(NZ * 32, gn.shape[2])

    @pl.loop(0, 2)
    def _(i):
        q[2 - 2 * i] = jnp.dot(tokens, w[1 - i, 2], preferred_element_type=F32).astype(BF16)

    q_copy.start()

    length = enc_len[0]

    kvs, seen = (kva, kvb, kvc), (5, 1, 1)
    kv_sems = ((kva_send, kva_recv), (kvb_send, kvb_recv), (kvc_send, kvc_recv))

    def kv_copy(units, u):
        kv, (ssem, rsem) = kvs[units], kv_sems[units]
        return remote(kv.at[2, u], kv.at[1, u], ssem.at[u], rsem.at[u], peers[2])

    def help_copy(units, side):
        kv, there = kvs[units], seen[units]
        return remote(
            kv.at[side, there + 1],
            kv.at[side, there],
            as_send.at[units, side],
            as_recv.at[units, side],
            peers[6 if side else 1],
        )

    def project(units, u, rows, sides=(2, 0)):
        kv = kvs[units]
        for side in sides:

            @pl.loop(0, 2)
            def _(which):
                kv[side, u, which] = jnp.dot(
                    rows, w[side // 2, which], preferred_element_type=F32
                ).astype(BF16)

            if side == 2:
                kv_copy(units, u).start()

    def assist(units, rows):
        kv, here = kvs[units], seen[units] + 1
        for side in (1, 0):

            @pl.loop(0, 2)
            def _(which):
                kv[side, here, which] = jnp.dot(rows, w2[side, which], preferred_element_type=F32).astype(BF16)

            help_copy(units, side).start()

    def attend(slots, last=False):
        keys, values, index = [], [], []
        for units, u, block, start in slots:
            kv = kvs[units]
            if not isinstance(u, int) or u < seen[units]:
                kv_copy(units, u).wait_recv()
            else:
                help_copy(units, 0).wait_recv()
                help_copy(units, 1).wait_recv()
            for side, row in ((0, y), (1, yn)):
                size = kv.shape[3]
                keys.append(kv[side, u, 0])
                values.append(kv[side, u, 1])
                base = (row * NZ + block) * 128 + start
                index.append(lax.broadcasted_iota(jnp.int32, (size, 1), 0) + base)
        keys = jnp.concatenate(keys, axis=0)
        values_t = jnp.concatenate(values, axis=0).T
        valid = jnp.broadcast_to(jnp.concatenate(index, axis=0), (keys.shape[0], 512)) < length

        def head(h, v_h):
            s = jnp.dot(keys, qtm[h], preferred_element_type=F32)
            s = jnp.where(valid, s, NEG)
            old = mx[h]
            new = jnp.maximum(old, jnp.max(s, axis=0, keepdims=True))
            p = jnp.exp(s - new)
            scale = jnp.exp(old - new)
            total = scale * sm[h] + jnp.sum(p, axis=0, keepdims=True)
            summed = scale * acc[h] + jnp.dot(v_h, p.astype(BF16), preferred_element_type=F32)
            if last:
                return (summed * (1.0 / total)).astype(BF16)
            mx[h] = new
            sm[h] = total
            acc[h] = summed

        heads = [lambda h=h: head(h, values_t[64 * h : 64 * h + 64]) for h in range(4)]
        if last:
            return heads
        for run in heads:
            run()

    def block_of(u):
        return (z + NZ + sign * ((u + 1) // 2) * (1 - 2 * (u % 2))) % NZ

    ends = {1: (0, 96), 2: (96, 32)}

    def end_rows(units):
        return gm[(z + NZ - 3 * sign) % NZ, pl.ds(*ends[units]), :]

    def end_slots(units):
        start = ends[units][0]
        return [(units, 0, (z + NZ - 3 * sign) % NZ, start), (units, 1, (z + 4) % NZ, start)]

    before = {
        1: lambda: (serve(1, 7), got_y(3), got_x(6)),
        2: lambda: (serve(1, 8), serve(0, 8), got_x(4), serve(1, 9), serve(0, 9), got_x(7)),
        3: lambda: (got_x(5), serve(0, 10), serve(1, 10), serve(0, 11), serve(1, 11)),
    }

    @pl.loop(0, 4)
    def _(u):
        for at, take in before.items():

            @pl.when(u == at)
            def _():
                take()

        project(0, u, gm[block_of(u)])

        @pl.when(u == 0)
        def _():
            q_copy.wait_recv()
            first = jnp.where(y == 0, q[0], q[1])
            second = jnp.where(y == 0, q[1], q[0])
            qt = jnp.concatenate([first.T, second.T], axis=1)
            column = lax.broadcasted_iota(jnp.int32, (256, 512), 0)
            for h in range(4):
                qtm[h] = jnp.where(column // HEAD_DIM == h, qt, jnp.zeros_like(qt))

        @pl.when(u > 0)
        def _():
            attend([(0, u - 1, block_of(u - 1), 0)])

    serve(1, 12)
    serve(0, 12)
    for t in (4, 5, 6, 7):
        wc(t, True).wait_recv()
    assist(0, gm[block_of(3)])
    attend([(0, 3, block_of(3), 0)])
    serve(1, 13)
    serve(0, 13)
    got_x(3)
    project(0, 4, gm[block_of(4)])
    attend([(0, 5, (z + NZ + 3 * sign) % NZ, 0)])
    attend([(0, 4, block_of(4), 0)])
    serve(0, 14)
    rows = end_rows(1)
    assist(1, rows)
    project(1, 0, rows)
    serve(0, 15)
    rows = end_rows(2)
    assist(2, rows)
    project(2, 0, rows, (2,))
    attend(end_slots(1))
    project(2, 0, rows, (0,))

    heads = attend(end_slots(2), True)

    def ctx_copy(pair):
        return remote(ctx.at[2, pair], ctx.at[1, pair], ctx_sem.at[0, pair], ctx_sem.at[1, pair], peers[2])

    for pair in (0, 1):
        full = jnp.concatenate([heads[2 * pair](), heads[2 * pair + 1]()], axis=0)
        low, high = full[:, :256].T, full[:, 256:].T
        ctx[2, pair] = jnp.where(y == 0, high, low)
        ctx_copy(pair).start()
        both_ctx[:, pl.ds(128 * pair, 128)] = jnp.where(y == 0, low, high)
    wc(3, True).wait_recv()
    for pair in (0, 1):
        ctx_copy(pair).wait_recv()
        both_ctx[:, pl.ds(256 + 128 * pair, 128)] = ctx[1, pair]

    orders = []
    for long in ((0, 1), (2, 3)):
        short = (2, 3) if long[0] == 0 else (0, 1)
        order = [(quarter, 4) for quarter in long]
        for far in (3, 2, 1):
            order += [(quarter, far) for quarter in short + long]
        orders.append(order)
    n_rs = len(orders[0])

    def rs_copy(d, i):
        return remote(rs_send.at[d, i], rs_recv.at[d, i], rss.at[d, i], rsr.at[d, i], ring[d])

    def term_of(owner, quarter):
        rows = both_ctx[pl.ds(pl.multiple_of(owner * 32, 32), 32), :]
        cols = pl.ds(quarter * 1024, 1024)
        return jnp.dot(rows[:, :256], wo[0, :, cols], preferred_element_type=F32) + jnp.dot(
            rows[:, 256:], wo[1, :, cols], preferred_element_type=F32
        )

    for i in range(n_rs):
        for d in (0, 1):
            quarter, far = orders[d][i]
            term = term_of((z + (far if d == 0 else NZ - far)) % NZ, quarter)
            if (quarter, far + 1) in orders[d]:
                k = orders[d].index((quarter, far + 1))
                rs_copy(d, k).wait_recv()
                term = term + rs_recv[d, k].astype(F32)
            rs_send[d, i] = term.astype(BF16)
            rs_copy(d, i).start()
    terms = [term_of(z, quarter) for quarter in range(4)]
    live = lax.broadcasted_iota(jnp.int32, (32, 1024), 0) + (y * NZ + z) * 32 < dec_len[0]
    for i in range(n_rs - 4, n_rs):
        for d in (0, 1):
            rs_copy(d, i).wait_recv()
            quarter = orders[d][i][0]
            terms[quarter] = terms[quarter] + rs_recv[d, i].astype(F32)
    for quarter in range(4):
        out_ref[:, pl.ds(quarter * 1024, 1024)] = jnp.where(live, terms[quarter], 0.0).astype(BF16)

    for d in (0, 1):
        for i in range(len(ITEMS[d])):
            z_copy(d, i, False).wait_send()
        for i in range(n_rs):
            rs_copy(d, i).wait_send()
    for t in range(8):
        for k in (0, 1):
            if t not in (4, 5):
                wy(t, k).wait_send()
            wx(t, k).wait_send()
        if t in (4, 5):
            wnear(t).wait_send()
        wc(t).wait_send()
    q_copy.wait_send()
    for pair in (0, 1):
        ctx_copy(pair).wait_send()
    for u in range(5):
        kv_copy(0, u).wait_send()
    for units in (1, 2):
        kv_copy(units, 0).wait_send()
    for units in range(3):
        for side in (0, 1):
            help_copy(units, side).wait_send()


def shards(enc_hidden, enc_gain, dec_hidden, dec_gain, w_query, w_key, w_value, w_out, enc_length, dec_length):
    width = w_query.shape[0]
    rows = dec_hidden.shape[0]
    anywhere = pl.BlockSpec(memory_space=pl.ANY)
    dma = pltpu.SemaphoreType.DMA
    return pl.pallas_call(
        kernel,
        out_shape=(
            pltpu.VMEM(enc_hidden.shape, BF16),
            pltpu.VMEM((rows, width), BF16),
        ),
        in_specs=[anywhere] * 10,
        out_specs=(pl.BlockSpec(memory_space=pltpu.VMEM), pl.BlockSpec(memory_space=pltpu.VMEM)),
        scratch_shapes=[
            pltpu.SMEM((1,), jnp.int32),
            pltpu.SMEM((1,), jnp.int32),
            pltpu.VMEM((160, width), BF16),
            pltpu.VMEM((2, 1, width), F32),
            pltpu.VMEM((NZ, 32, width), BF16),
            pltpu.VMEM((NZ, 128, width), BF16),
            pltpu.VMEM((2, 3, width, 256), BF16),
            pltpu.VMEM((2, 2, width, 256), BF16),
            pltpu.VMEM((2, 256, width), BF16),
            pltpu.VMEM((3, 7, 2, 128, 256), BF16),
            pltpu.VMEM((3, 3, 2, 96, 256), BF16),
            pltpu.VMEM((3, 3, 2, 32, 256), BF16),
            pltpu.VMEM((3, 256, 256), BF16),
            pltpu.VMEM((4, 256, 512), BF16),
            pltpu.VMEM((4, 64, 512), F32),
            pltpu.VMEM((4, 1, 512), F32),
            pltpu.VMEM((4, 1, 512), F32),
            pltpu.VMEM((3, 2, 256, 128), BF16),
            pltpu.VMEM((256, 512), BF16),
            pltpu.VMEM((2, 14, 32, width // 4), BF16),
            pltpu.VMEM((2, 14, 32, width // 4), BF16),
            pltpu.SemaphoreType.REGULAR((3,)),
            dma((11,)),
            dma((2, 16)),
            dma((2, 16)),
            dma((8, 2)),
            dma((8, 2)),
            dma((8,)),
            dma((8,)),
            dma((8, 2)),
            dma((8, 2)),
            dma((8,)),
            dma((8,)),
            dma((2,)),
            dma((2, 2)),
            dma((5,)),
            dma((5,)),
            dma((1,)),
            dma((1,)),
            dma((1,)),
            dma((1,)),
            dma((3, 2)),
            dma((3, 2)),
            dma((2, 14)),
            dma((2, 14)),
        ],
        compiler_params=pltpu.CompilerParams(
            collective_id=0, has_side_effects=True, vmem_limit_bytes=60 * 1024 * 1024
        ),
        name="cross_attention",
    )(
        enc_length,
        dec_length,
        enc_hidden,
        enc_gain.reshape(1, width),
        dec_hidden,
        dec_gain.reshape(1, width),
        w_query,
        w_key,
        w_value,
        w_out,
    )


def solution(mesh):
    torus = Mesh(mesh.devices.reshape(4, 2, 2, 2, NZ), ROWS)
    tensor = ("yl", "z")
    dp = ("x", "yh", "c")
    in_specs = (
        P(ROWS, None),
        P(),
        P(ROWS, None),
        P(),
        P(None, tensor),
        P(None, tensor),
        P(None, tensor),
        P(tensor, None),
        P(dp),
        P(dp),
    )
    out_specs = (P(ROWS, None), P(ROWS, None))
    return jax.shard_map(shards, mesh=torus, in_specs=in_specs, out_specs=out_specs, check_vma=False)
```

```python
import functools

import jax
import jax.numpy as jnp
from jax import lax
from jax.experimental import pallas as pl
from jax.experimental.pallas import tpu as pltpu
from jax.sharding import Mesh
from jax.sharding import PartitionSpec as P

HEAD_DIM = 64
MESH = pl.DeviceIdType.MESH
NZ = 8
NEG = -1e30
ROWS = ("x", "yh", "c", "yl", "z")
BF16, F32 = jnp.bfloat16, jnp.float32

OUTER = (
    [("n", 0, 0), ("m", 0, 0), ("n", 1, 0), ("m", 0, 1), ("n", 2, 0), ("m", 0, 2), ("n", 3, 4), ("m", 0, 3)]
    + [("m", 1, p) for p in range(4)]
    + [("m", 2, p) for p in range(4)]
)
INNER = (
    [("n", 0, 0), ("w", 0, 0), ("n", 1, 0), ("w", 0, 1), ("n", 2, 0), ("m", 0, 0), ("n", 3, 5)]
    + [("m", 0, p) for p in (1, 2, 3)]
    + [("m", 1, p) for p in range(4)]
)
ITEMS = (OUTER, INNER)


def schedule(d):
    after, last = {}, -1
    for i, (kind, hop, piece) in enumerate(ITEMS[d]):
        if hop:
            last = max(last, ITEMS[1 - d].index((kind, hop - 1, piece % 4 if kind == "m" else 0)))
        after.setdefault(last, []).append(i)
    return after


def rms_norm(values, gain):
    wide = values.astype(F32)
    mean_sq = jnp.mean(wide * wide, axis=-1, keepdims=True)
    return (wide * lax.rsqrt(mean_sq + 1e-06) * gain).astype(BF16)


def kernel(
    enc_len_hbm, dec_len_hbm, enc_hbm, encg_hbm, dec_hbm, decg_hbm, wq_hbm, wk_hbm, wv_hbm, wo_hbm, mem_out, out_ref,
    enc_len, dec_len, raw, gain, gn, gm, w, w2, wo, kva, kvb, kvc, q, qtm, acc, mx, sm, ctx, both_ctx, rs_send, rs_recv,
    ready, loc, z_send, z_recv, wy_send, wy_recv, xa_send, xa_recv, xb_send, xb_recv, c_send, c_recv,
    q_sem, ctx_sem, kva_send, kva_recv, kvb_send, kvb_recv, kvc_send, kvc_recv, as_send, as_recv, rss, rsr,
):
    x, c = lax.axis_index("x"), lax.axis_index("c")
    y, z = lax.axis_index("yl"), lax.axis_index("z")
    yh = lax.axis_index("yh")
    yn, cn = 1 - y, 1 - c
    xa, xb = x + 1 - 2 * (x % 2), 3 - x
    right, left = (z + 1) % NZ, (z + NZ - 1) % NZ
    sign = 1 - 2 * (z % 2)
    inner, outer = z + sign, (z + NZ - sign) % NZ
    ring = ({"z": right}, {"z": left})
    peers = ({"z": outer}, {"z": inner}, {"yl": yn}, {"x": xa}, {"x": xb}, {"c": cn}, {"yl": yn, "z": inner})
    peers += ({"yl": yn, "yh": 1 - yh},)

    barrier = pltpu.get_barrier_semaphore()

    def greet(*to):
        for peer in to:
            pl.semaphore_signal(barrier, inc=1, device_id=peer, device_id_type=MESH)

    def answer(which, peer):
        pl.semaphore_signal(ready.at[which], inc=1, device_id=peer, device_id_type=MESH)

    greet(*peers[:3], *peers[6:])
    pl.when(c == 0)(lambda: greet(peers[5]))
    pl.when(x == 0)(lambda: greet(peers[3], peers[4]))
    pl.when(x == 1)(lambda: greet(peers[4]))
    pl.when(x == 3)(lambda: greet(peers[3]))

    enters = [
        pltpu.make_async_copy(dec_hbm, raw.at[pl.ds(0, 32), :], loc.at[0]),
        pltpu.make_async_copy(decg_hbm, gain.at[0], loc.at[1]),
        pltpu.make_async_copy(enc_hbm.at[pl.ds(0, 32), :], raw.at[pl.ds(32, 32), :], loc.at[2]),
        pltpu.make_async_copy(encg_hbm, gain.at[1], loc.at[3]),
        pltpu.make_async_copy(enc_hbm.at[pl.ds(32, 96), :], raw.at[pl.ds(64, 96), :], loc.at[8]),
    ]
    local = [
        pltpu.make_async_copy(wk_hbm, w.at[0, 0], loc.at[4]),
        pltpu.make_async_copy(wv_hbm, w.at[0, 1], loc.at[5]),
        pltpu.make_async_copy(wq_hbm, w.at[0, 2], loc.at[6]),
        pltpu.make_async_copy(wo_hbm, wo.at[0], loc.at[7]),
        pltpu.make_async_copy(enc_len_hbm, enc_len, loc.at[9]),
        pltpu.make_async_copy(dec_len_hbm, dec_len, loc.at[10]),
    ]
    for copy in enters:
        copy.start()
    enters[0].wait()
    enters[1].wait()
    gn[z] = rms_norm(raw[pl.ds(0, 32), :], gain[0])
    enters[2].wait()
    enters[3].wait()

    def norm_piece(p):
        gm[z, pl.ds(32 * p, 32), :] = rms_norm(raw[pl.ds(32 + 32 * p, 32), :], gain[1])

    norm_piece(0)
    pl.semaphore_wait(barrier, 5 + c + x - 2 * (x // 3))

    def remote(src, dst, ssem, rsem, peer):
        return pltpu.make_async_remote_copy(
            src_ref=src, dst_ref=dst, send_sem=ssem, recv_sem=rsem, device_id=peer, device_id_type=MESH
        )

    hbm = (wk_hbm, wv_hbm, wq_hbm, wo_hbm)

    def partner_of(t, at):
        return at + 1 - 2 * (at % 2) if t in (1, 3, 4, 6) else 3 - at

    def held(t, at, other=False):
        flip = 1 - yh if other else yh
        return c * 4 + at + flip * (partner_of(t, at) - at)


    def part(t, e, n=1):
        if t == 3:
            return wo.at[1, pl.ds(e * 32, n * 32), :]
        rows = pl.ds(e * 512, n * 512)
        return w.at[1, t, rows, :] if t < 3 else w2.at[t // 2 - 2, t % 2, rows, :]

    def z_ref(kind, owner, piece):
        if kind == "n":
            return gn.at[owner] if piece == 0 else gn.at[owner, pl.ds(16 * (piece - 4), 16), :]
        return gm.at[owner, pl.ds(32 * piece, 32), :]

    def z_copy(d, i, receive):
        kind, hop, piece = ITEMS[d][i]
        if kind == "w":
            e = held(4 + piece, x)
            src, dst = hbm[piece].at[pl.ds(e * 512, 512), :], part(4 + piece, e)
        else:
            away = sign if d == (1 if receive else 0) else -sign
            src = dst = z_ref(kind, (z + NZ + away * (hop + (1 if receive else 0))) % NZ, piece)
        return remote(src, dst, z_send.at[d, i], z_recv.at[d, i], peers[d])

    plan = (schedule(0), schedule(1))

    def z_issue(d, k):
        for i in plan[d].get(k, ()):
            z_copy(d, i, False).start()

    def serve(d, k):
        z_copy(d, k, True).wait_recv()
        z_issue(1 - d, k)

    def wy(t, far, receive=False):
        e = held(t, x, receive and far == 1)
        size = 32 if t == 3 else 512
        src = hbm[t].at[pl.ds(e * size, size), :] if t < 4 else part(t - 2, e)
        return remote(src, part(t, e), wy_send.at[t, far], wy_recv.at[t, far], peers[7 if far else 2])

    def wx(t, k, receive=False):
        if t in (4, 5):
            near, at, peer = ((xa, xb, 4), (xb, xa, 3))[t - 4]
            e = held(t, (3 - xa if k else at) if receive else (near if k else x))
        else:
            at, peer = (xb, 4) if t in (1, 3, 6) else (xa, 3)
            e = held(t, at if receive else x, k == 1)
        return remote(part(t, e), part(t, e), xb_send.at[t, k], xb_recv.at[t, k], peers[peer])

    def wnear(t, receive=False):
        at, peer = ((xa, 3), (xb, 4))[t - 4]
        r = part(t, held(t, at if receive else x))
        return remote(r, r, xa_send.at[t], xa_recv.at[t], peers[peer])

    def wc(t, receive=False):
        r = part(t, 4 * (cn if receive else c), 4)
        return remote(r, r, c_send.at[t], c_recv.at[t], peers[5])

    def send_y(t):
        wy(t, 0).start()
        wy(t, 1).start()

    def got_y(t):
        for k in (0, 1):
            wy(t, k, True).wait_recv()
        for k in (0, 1):
            wx(t, k).start()

    def got_z(t):
        send_y(t + 2)
        wx(t, 0).start()
        wnear(t).start()

    def got_near(t):
        wnear(t, True).wait_recv()
        wx(t, 1).start()

    def got_x(t):
        for k in (0, 1):
            wx(t, k, True).wait_recv()
        wc(t).start()

    for d in (0, 1):
        z_issue(d, -1)
    for t in range(3):
        send_y(t)
    pl.when(c == 1)(lambda: answer(0, peers[5]))
    pl.when(x == 1)(lambda: answer(1, peers[3]))
    pl.when(x == 3)(lambda: answer(2, peers[4]))

    @pl.when(x == 2)
    def _():
        answer(1, peers[3])
        answer(2, peers[4])
    for copy in local:
        copy.start()
    enters[4].wait()

    @pl.loop(1, 4)
    def _(p):
        norm_piece(p)

    mem_out[...] = gm[z]
    mx[...] = jnp.full_like(mx, NEG)
    sm[...] = jnp.zeros_like(sm)
    acc[...] = jnp.zeros_like(acc)

    def both(k):
        serve(0, k)
        serve(1, k)

    both(0)

    @pl.when(x // 2 == 0)
    def _():
        pl.semaphore_wait(ready.at[2], 1)

    pl.when(x % 3 == 0)(lambda: pl.semaphore_wait(ready.at[1], 1))
    got_y(0)
    got_y(1)
    both(1)
    got_z(4)
    got_y(2)
    both(2)
    both(3)
    got_z(5)
    send_y(3)
    got_y(6)
    pl.when(c == 0)(lambda: pl.semaphore_wait(ready.at[0], 1))
    got_x(0)
    got_near(4)
    both(4)
    got_x(1)
    got_y(7)
    both(5)
    got_x(2)
    both(6)
    got_near(5)
    serve(0, 7)
    for copy in local:
        copy.wait()
    for t in (2, 0, 1):
        wc(t, True).wait_recv()

    q_copy = remote(q.at[2], q.at[1], q_sem.at[0], q_sem.at[1], peers[2])
    tokens = gn[...].reshape(NZ * 32, gn.shape[2])

    @pl.loop(0, 2)
    def _(i):
        q[2 - 2 * i] = jnp.dot(tokens, w[1 - i, 2], preferred_element_type=F32).astype(BF16)

    q_copy.start()

    length = enc_len[0]

    kvs, seen = (kva, kvb, kvc), (5, 1, 1)
    kv_sems = ((kva_send, kva_recv), (kvb_send, kvb_recv), (kvc_send, kvc_recv))

    def kv_copy(units, u):
        kv, (ssem, rsem) = kvs[units], kv_sems[units]
        return remote(kv.at[2, u], kv.at[1, u], ssem.at[u], rsem.at[u], peers[2])

    def help_copy(units, side):
        kv, there = kvs[units], seen[units]
        return remote(
            kv.at[side, there + 1],
            kv.at[side, there],
            as_send.at[units, side],
            as_recv.at[units, side],
            peers[6 if side else 1],
        )

    def project(units, u, rows, sides=(2, 0)):
        kv = kvs[units]
        for side in sides:

            @pl.loop(0, 2)
            def _(which):
                kv[side, u, which] = jnp.dot(
                    rows, w[side // 2, which], preferred_element_type=F32
                ).astype(BF16)

            if side == 2:
                kv_copy(units, u).start()

    def assist(units, rows):
        kv, here = kvs[units], seen[units] + 1
        for side in (1, 0):

            @pl.loop(0, 2)
            def _(which):
                kv[side, here, which] = jnp.dot(rows, w2[side, which], preferred_element_type=F32).astype(BF16)

            help_copy(units, side).start()

    def attend(slots, last=False):
        keys, values, index = [], [], []
        for units, u, block, start in slots:
            kv = kvs[units]
            if not isinstance(u, int) or u < seen[units]:
                kv_copy(units, u).wait_recv()
            else:
                help_copy(units, 0).wait_recv()
                help_copy(units, 1).wait_recv()
            for side, row in ((0, y), (1, yn)):
                size = kv.shape[3]
                keys.append(kv[side, u, 0])
                values.append(kv[side, u, 1])
                base = (row * NZ + block) * 128 + start
                index.append(lax.broadcasted_iota(jnp.int32, (size, 1), 0) + base)
        keys = jnp.concatenate(keys, axis=0)
        values_t = jnp.concatenate(values, axis=0).T
        valid = jnp.broadcast_to(jnp.concatenate(index, axis=0), (keys.shape[0], 512)) < length

        def head(h, v_h):
            s = jnp.dot(keys, qtm[h], preferred_element_type=F32)
            s = jnp.where(valid, s, NEG)
            old = mx[h]
            new = jnp.maximum(old, jnp.max(s, axis=0, keepdims=True))
            p = jnp.exp(s - new)
            scale = jnp.exp(old - new)
            total = scale * sm[h] + jnp.sum(p, axis=0, keepdims=True)
            summed = scale * acc[h] + jnp.dot(v_h, p.astype(BF16), preferred_element_type=F32)
            if last:
                return (summed * (1.0 / total)).astype(BF16)
            mx[h] = new
            sm[h] = total
            acc[h] = summed

        heads = [lambda h=h: head(h, values_t[64 * h : 64 * h + 64]) for h in range(4)]
        if last:
            return heads
        for run in heads:
            run()

    def block_of(u):
        return (z + NZ + sign * ((u + 1) // 2) * (1 - 2 * (u % 2))) % NZ

    ends = {1: (0, 96), 2: (96, 32)}

    def end_rows(units):
        return gm[(z + NZ - 3 * sign) % NZ, pl.ds(*ends[units]), :]

    def end_slots(units):
        start = ends[units][0]
        return [(units, 0, (z + NZ - 3 * sign) % NZ, start), (units, 1, (z + 4) % NZ, start)]

    before = {
        1: lambda: (serve(1, 7), got_y(3), got_x(6)),
        2: lambda: (serve(1, 8), serve(0, 8), got_x(4), serve(1, 9), serve(0, 9), got_x(7)),
        3: lambda: (got_x(5), serve(0, 10), serve(1, 10), serve(0, 11), serve(1, 11)),
    }

    @pl.loop(0, 4)
    def _(u):
        for at, take in before.items():

            @pl.when(u == at)
            def _():
                take()

        project(0, u, gm[block_of(u)])

        @pl.when(u == 0)
        def _():
            q_copy.wait_recv()
            first = jnp.where(y == 0, q[0], q[1])
            second = jnp.where(y == 0, q[1], q[0])
            qt = jnp.concatenate([first.T, second.T], axis=1)
            column = lax.broadcasted_iota(jnp.int32, (256, 512), 0)
            for h in range(4):
                qtm[h] = jnp.where(column // HEAD_DIM == h, qt, jnp.zeros_like(qt))

        @pl.when(u > 0)
        def _():
            attend([(0, u - 1, block_of(u - 1), 0)])

    serve(1, 12)
    serve(0, 12)
    for t in (4, 5, 6, 7):
        wc(t, True).wait_recv()
    assist(0, gm[block_of(3)])
    attend([(0, 3, block_of(3), 0)])
    serve(1, 13)
    serve(0, 13)
    got_x(3)
    project(0, 4, gm[block_of(4)])
    attend([(0, 5, (z + NZ + 3 * sign) % NZ, 0)])
    attend([(0, 4, block_of(4), 0)])
    serve(0, 14)
    rows = end_rows(1)
    assist(1, rows)
    project(1, 0, rows)
    serve(0, 15)
    rows = end_rows(2)
    assist(2, rows)
    project(2, 0, rows, (2,))
    attend(end_slots(1))
    project(2, 0, rows, (0,))

    heads = attend(end_slots(2), True)

    def ctx_copy(pair):
        return remote(ctx.at[2, pair], ctx.at[1, pair], ctx_sem.at[0, pair], ctx_sem.at[1, pair], peers[2])

    for pair in (0, 1):
        full = jnp.concatenate([heads[2 * pair](), heads[2 * pair + 1]()], axis=0)
        low, high = full[:, :256].T, full[:, 256:].T
        ctx[2, pair] = jnp.where(y == 0, high, low)
        ctx_copy(pair).start()
        both_ctx[:, pl.ds(128 * pair, 128)] = jnp.where(y == 0, low, high)
    wc(3, True).wait_recv()
    for pair in (0, 1):
        ctx_copy(pair).wait_recv()
        both_ctx[:, pl.ds(256 + 128 * pair, 128)] = ctx[1, pair]

    orders = []
    for long in ((0, 1), (2, 3)):
        short = (2, 3) if long[0] == 0 else (0, 1)
        order = [(quarter, 4) for quarter in long]
        for far in (3, 2, 1):
            order += [(quarter, far) for quarter in short + long]
        orders.append(order)
    n_rs = len(orders[0])

    def rs_copy(d, i):
        return remote(rs_send.at[d, i], rs_recv.at[d, i], rss.at[d, i], rsr.at[d, i], ring[d])

    def term_of(owner, quarter):
        rows = both_ctx[pl.ds(pl.multiple_of(owner * 32, 32), 32), :]
        cols = pl.ds(quarter * 1024, 1024)
        return jnp.dot(rows[:, :256], wo[0, :, cols], preferred_element_type=F32) + jnp.dot(
            rows[:, 256:], wo[1, :, cols], preferred_element_type=F32
        )

    for i in range(n_rs):
        for d in (0, 1):
            quarter, far = orders[d][i]
            term = term_of((z + (far if d == 0 else NZ - far)) % NZ, quarter)
            if (quarter, far + 1) in orders[d]:
                k = orders[d].index((quarter, far + 1))
                rs_copy(d, k).wait_recv()
                term = term + rs_recv[d, k].astype(F32)
            rs_send[d, i] = term.astype(BF16)
            rs_copy(d, i).start()
    terms = [term_of(z, quarter) for quarter in range(4)]
    live = lax.broadcasted_iota(jnp.int32, (32, 1024), 0) + (y * NZ + z) * 32 < dec_len[0]
    for i in range(n_rs - 4, n_rs):
        for d in (0, 1):
            rs_copy(d, i).wait_recv()
            quarter = orders[d][i][0]
            terms[quarter] = terms[quarter] + rs_recv[d, i].astype(F32)
    for quarter in range(4):
        out_ref[:, pl.ds(quarter * 1024, 1024)] = jnp.where(live, terms[quarter], 0.0).astype(BF16)

    for d in (0, 1):
        for i in range(len(ITEMS[d])):
            z_copy(d, i, False).wait_send()
        for i in range(n_rs):
            rs_copy(d, i).wait_send()
    for t in range(8):
        for k in (0, 1):
            if t not in (4, 5):
                wy(t, k).wait_send()
            wx(t, k).wait_send()
        if t in (4, 5):
            wnear(t).wait_send()
        wc(t).wait_send()
    q_copy.wait_send()
    for pair in (0, 1):
        ctx_copy(pair).wait_send()
    for u in range(5):
        kv_copy(0, u).wait_send()
    for units in (1, 2):
        kv_copy(units, 0).wait_send()
    for units in range(3):
        for side in (0, 1):
            help_copy(units, side).wait_send()


def shards(enc_hidden, enc_gain, dec_hidden, dec_gain, w_query, w_key, w_value, w_out, enc_length, dec_length):
    width = w_query.shape[0]
    rows = dec_hidden.shape[0]
    anywhere = pl.BlockSpec(memory_space=pl.ANY)
    dma = pltpu.SemaphoreType.DMA
    return pl.pallas_call(
        kernel,
        out_shape=(
            pltpu.VMEM(enc_hidden.shape, BF16),
            pltpu.VMEM((rows, width), BF16),
        ),
        in_specs=[anywhere] * 10,
        out_specs=(pl.BlockSpec(memory_space=pltpu.VMEM), pl.BlockSpec(memory_space=pltpu.VMEM)),
        scratch_shapes=[
            pltpu.SMEM((1,), jnp.int32),
            pltpu.SMEM((1,), jnp.int32),
            pltpu.VMEM((160, width), BF16),
            pltpu.VMEM((2, 1, width), F32),
            pltpu.VMEM((NZ, 32, width), BF16),
            pltpu.VMEM((NZ, 128, width), BF16),
            pltpu.VMEM((2, 3, width, 256), BF16),
            pltpu.VMEM((2, 2, width, 256), BF16),
            pltpu.VMEM((2, 256, width), BF16),
            pltpu.VMEM((3, 7, 2, 128, 256), BF16),
            pltpu.VMEM((3, 3, 2, 96, 256), BF16),
            pltpu.VMEM((3, 3, 2, 32, 256), BF16),
            pltpu.VMEM((3, 256, 256), BF16),
            pltpu.VMEM((4, 256, 512), BF16),
            pltpu.VMEM((4, 64, 512), F32),
            pltpu.VMEM((4, 1, 512), F32),
            pltpu.VMEM((4, 1, 512), F32),
            pltpu.VMEM((3, 2, 256, 128), BF16),
            pltpu.VMEM((256, 512), BF16),
            pltpu.VMEM((2, 14, 32, width // 4), BF16),
            pltpu.VMEM((2, 14, 32, width // 4), BF16),
            pltpu.SemaphoreType.REGULAR((3,)),
            dma((11,)),
            dma((2, 16)),
            dma((2, 16)),
            dma((8, 2)),
            dma((8, 2)),
            dma((8,)),
            dma((8,)),
            dma((8, 2)),
            dma((8, 2)),
            dma((8,)),
            dma((8,)),
            dma((2,)),
            dma((2, 2)),
            dma((5,)),
            dma((5,)),
            dma((1,)),
            dma((1,)),
            dma((1,)),
            dma((1,)),
            dma((3, 2)),
            dma((3, 2)),
            dma((2, 14)),
            dma((2, 14)),
        ],
        compiler_params=pltpu.CompilerParams(
            collective_id=0, has_side_effects=True, vmem_limit_bytes=60 * 1024 * 1024
        ),
        name="cross_attention",
    )(
        enc_length,
        dec_length,
        enc_hidden,
        enc_gain.reshape(1, width),
        dec_hidden,
        dec_gain.reshape(1, width),
        w_query,
        w_key,
        w_value,
        w_out,
    )


def solution(mesh):
    torus = Mesh(mesh.devices.reshape(4, 2, 2, 2, NZ), ROWS)
    tensor = ("yl", "z")
    dp = ("x", "yh", "c")
    in_specs = (
        P(ROWS, None),
        P(),
        P(ROWS, None),
        P(),
        P(None, tensor),
        P(None, tensor),
        P(None, tensor),
        P(tensor, None),
        P(dp),
        P(dp),
    )
    out_specs = (P(ROWS, None), P(ROWS, None))
    return jax.shard_map(shards, mesh=torus, in_specs=in_specs, out_specs=out_specs, check_vma=False)
```
